512 devices in a mesh: mem: 32 (over y, x), space: 16 (over z, core).
Axes of the slice: x: 4, y: 8, z: 8, core: 2. Of those that a mesh axis runs over, the one named last changes fastest.
Arguments:
- ensemble: float32 [384, 3, 64, 1024], P('mem', None, 'space'), may hold values from -1.8 to 1.8
- sea_depth: float32 [64, 1024], P('space'), may hold values from 0.5 to 2
- ocean_mask: int32 [64, 1024], P('space'), may hold values 0 or 1
- observed_cells: int32 [16, 128], P('space'), may hold values from 0 to 4095
- observed_values: float32 [16, 128], P('space'), may hold values from -6 to 6
- observed_error: float32 [16, 128], P('space'), may hold values from 0.5 to 2
Outputs:
- analysis: float32 [384, 3, 64, 1024], P('mem', None, 'space')
The draws below stay inside these ranges and needn't reach their ends.
Inputs may be any that keep to these rules, and one draw needn't show every extreme that they name: `observed_cells`: indices are local to the slab; an observation may repeat a cell.
All inputs are finite; a program needn't handle non-finite values. No bound on the sum of `ocean_mask` on one device may be relied on, other than what follows from the above.
Results may differ from the reference program's by a relative error of at most 0.00021.
Values sent between devices are 32-bit elements; how exact they have to be, the bound alone decides.
No kernel may reach another device: no remote copies, remote signals or barrier semaphores. Data moves between devices by JAX's collectives and lax.ppermute only.
A program may use at most 64 MiB of HBM per device.

```python
import math
import jax
import jax.numpy as jnp
from jax import lax

ENS = 384
CX = 4
NY = 1024
OBS = 128
STEPS = 3
NS_ITERS = 6
NX = 64
N_SPACE = 16


def with_ends(drawn, own_key, least, high):
    dims = drawn.shape
    index_at = [jax.random.randint(jax.random.fold_in(own_key, axis), (), 0, dims[axis]) for axis in range(len(dims))]
    drawn = drawn.at[tuple(index_at)].set(least)
    longest = dims.index(max(dims))
    index_at[longest] = (index_at[longest] + 1) % dims[longest]
    return drawn.at[tuple(index_at)].set(high)


def block_scale(rng, extent, split, low, top_value):
    loudness, own = 1.0, jax.random.fold_in(rng, 6)
    for dim, shards_of in split:
        steps = jnp.exp(jax.random.uniform(jax.random.fold_in(own, dim), (shards_of,), jnp.float32, low / len(split), top_value / len(split)))
        loudness = loudness * jnp.repeat(steps, extent[dim] // shards_of).reshape([-1 if axis == dim else 1 for axis in range(len(extent))])
    return loudness


def centred(own_key, shape, width, reach, cuts=(), kind=jnp.bfloat16):
    array = jax.random.normal(own_key, shape, jnp.float32) * width
    if len(cuts) > 0:
        array = block_scale(own_key, shape, cuts, -0.22, 0.18) * array
    return jnp.clip(array, min=-reach, max=reach).astype(kind)


def setup_inputs(seed: int = 0) -> dict:
    key_list = jax.random.split(jax.random.key(seed), 7)
    return {
        "ensemble": centred(key_list[0], (ENS, 3, NX, NY), 0.3, 1.8, ((0, 32), (2, 16)), jnp.float32),
        "sea_depth": jnp.clip(jnp.exp(math.log(2.0) - 1.3862944 * jax.random.uniform(key_list[1], (NX, NY), jnp.float32) ** block_scale(key_list[1], (NX, NY), ((0, 16),), -0.2, 0.2)), 0.5, 2.0),
        "ocean_mask": with_ends((jax.random.randint(key_list[2], (NX, NY), 0, 10) < 9).astype(jnp.int32), jax.random.fold_in(key_list[2], 1), 0, 1),
        "observed_cells": with_ends(jax.random.randint(key_list[3], (N_SPACE, OBS), 0, CX * NY), jax.random.fold_in(key_list[3], 1), 0, (CX * NY) - 1).astype(jnp.int32),
        "observed_values": centred(key_list[4], (N_SPACE, OBS), 1.0, 6.0, ((0, 16),), jnp.float32),
        "observed_error": jnp.clip(jnp.exp(math.log(2.0) - 1.3862944 * jax.random.uniform(key_list[5], (N_SPACE, OBS), jnp.float32) ** block_scale(key_list[5], (N_SPACE, OBS), ((0, 16),), -0.2, 0.2)), 0.5, 2.0),
    }


GRAV = 1.0
DT = 0.3
VISC = 0.1

def east(field):
    return (jnp.roll(field, -1, axis=-2) - jnp.roll(field, 1, axis=-2)) * 0.5

def north(field):
    return (jnp.roll(field, -1, axis=-1) - jnp.roll(field, 1, axis=-1)) * 0.5

def spread(field):
    return jnp.roll(field, -1, axis=-2) + jnp.roll(field, 1, axis=-2) + jnp.roll(field, 1, axis=-1) + jnp.roll(field, -1, axis=-1) - 4.0 * field

def advance(state, sea_depth, ocean, coriolis):
    height = state[:, 0]
    along = state[:, 1]
    across = state[:, 2]
    total = sea_depth + height
    fresh = height - DT * (east(total * along) + north(total * across))
    tend_along = GRAV * east(fresh) + along * east(along) + across * north(along) - coriolis * across
    tend_across = GRAV * north(fresh) + along * east(across) + across * north(across) + coriolis * along
    along_new = (along - DT * tend_along + DT * VISC * spread(along)) * ocean
    across_new = (across - DT * tend_across + DT * VISC * spread(across)) * ocean
    return jnp.stack([fresh, along_new, across_new], axis=1)

def inverse_root(matrix, sweeps):
    norm_scale = jnp.sqrt(jnp.sum(matrix * matrix))
    identity = jnp.eye(matrix.shape[0], dtype=jnp.float32)
    iterate = matrix / norm_scale
    inverse = identity
    for sweep_index in range(sweeps):
        factor = 1.5 * identity - 0.5 * jnp.dot(inverse, iterate, precision=lax.Precision.HIGHEST)
        iterate = jnp.dot(iterate, factor, precision=lax.Precision.HIGHEST)
        inverse = jnp.dot(factor, inverse, precision=lax.Precision.HIGHEST)
    return inverse / jnp.sqrt(norm_scale)

def reference(ensemble, sea_depth, ocean_mask, observed_cells, observed_values, observed_error):
    ocean = ocean_mask.astype(jnp.float32)
    coriolis = 0.05 + 0.1 * jnp.arange(NY, dtype=jnp.float32) / NY
    state = ensemble
    for step_index in range(STEPS):
        state = advance(state, sea_depth, ocean, coriolis)
    members = state.shape[0]
    heights = state[:, 0].reshape(members, N_SPACE, CX * NY)
    picked = jax.vmap(lambda rows, where: jnp.take(rows, where, axis=1), in_axes=(1, 0), out_axes=1)(heights, observed_cells.astype(jnp.int32))
    picked = picked.reshape(members, N_SPACE * OBS)
    errors = observed_error.reshape(N_SPACE * OBS)
    values = observed_values.reshape(N_SPACE * OBS)
    hmean = lax.optimization_barrier(jnp.mean(picked, axis=0))
    scaled = (picked - hmean) / errors
    misfit = (values - hmean) / errors
    gram = jnp.dot(scaled, scaled.T, precision=lax.Precision.HIGHEST)
    drive = jnp.dot(scaled, misfit, precision=lax.Precision.HIGHEST)
    identity = jnp.eye(members, dtype=jnp.float32)
    weights = inverse_root(identity + gram / (members - 1), NS_ITERS)
    mean_weight = jnp.dot(weights, jnp.dot(weights, drive, precision=lax.Precision.HIGHEST), precision=lax.Precision.HIGHEST) / (members - 1)
    combined = weights + mean_weight[:, None]
    flat = state.reshape(members, -1)
    center = lax.optimization_barrier(jnp.mean(flat, axis=0))
    result = center + jnp.dot(combined.T, flat - center, precision=lax.Precision.HIGHEST)
    return result.reshape(state.shape)
```

```python
import functools

import jax
import jax.numpy as jnp
from jax import lax
from jax.experimental import pallas as pl
from jax.experimental.pallas import tpu as pltpu
from jax.sharding import Mesh
from jax.sharding import PartitionSpec as P

STEPS = 3
NS_ITERS = 6
MEM = ("mem_0", "mem_1")

GRAV = 1.0
DT = 0.3
VISC = 0.1

LANES = 128
GROUP = 16
HALO = 2 * STEPS


def ring(axis, turn):
    count = lax.axis_size(axis)
    return [(i, (i + turn) % count) for i in range(count)]


def halves(x):
    top = x.astype(jnp.bfloat16)
    return top, (x - top.astype(jnp.float32)).astype(jnp.bfloat16)


def product(a, b, contract=((1,), (0,))):
    left = jnp.concatenate([a[0], a[0], a[1]], axis=contract[0][0])
    right = jnp.concatenate([b[0], b[1], b[0]], axis=contract[1][0])
    return lax.dot_general(left, right, (contract, ((), ())), preferred_element_type=jnp.float32)


def room(mebibytes):
    return pltpu.CompilerParams(vmem_limit_bytes=mebibytes << 20)


def forecast_kernel(cells, wide_ref, coriolis_ref, out_ref, a_ref, b_ref, fresh_ref):
    rows, _, columns = wide_ref.shape
    members = a_ref.shape[2]
    rows_here = rows - 2 * HALO
    coriolis = coriolis_ref[...] * DT
    parts = [slice(at, min(at + 8, members)) for at in range(0, members, 8)]
    depth_at = slice(3 * members, 3 * members + 1)
    ocean_at = slice(3 * members + 1, 3 * members + 2)

    def north(x):
        return pltpu.roll(x, columns - 1, 1)

    def south(x):
        return pltpu.roll(x, 1, 1)

    def unpack(r, carry):
        for f in range(3):
            b_ref[f, r] = wide_ref[r, f * members : (f + 1) * members, :]
        return carry

    lax.fori_loop(0, rows, unpack, 0)

    for step in range(STEPS):
        source, target = (b_ref, a_ref) if step % 2 == 0 else (a_ref, b_ref)
        low = 2 * step

        def height_row(r, carry, source=source):
            depth_above = wide_ref[r + 1, depth_at]
            depth_below = wide_ref[r - 1, depth_at]
            depth = wide_ref[r, depth_at]
            for m in parts:
                above = (depth_above + source[0, r + 1, m]) * source[1, r + 1, m]
                below = (depth_below + source[0, r - 1, m]) * source[1, r - 1, m]
                height = source[0, r, m]
                across = (depth + height) * source[2, r, m]
                fresh_ref[r, m] = height - (0.5 * DT) * (
                    (above - below) + (north(across) - south(across))
                )
            return carry

        lax.fori_loop(low + 1, rows - low - 1, height_row, 0)

        def flow_row(r, carry, source=source, target=target):
            ocean = wide_ref[r, ocean_at]
            for m in parts:
                u, v = source[1, r, m], source[2, r, m]
                ue, uw = source[1, r + 1, m], source[1, r - 1, m]
                un, us = north(u), south(u)
                tend = GRAV * (fresh_ref[r + 1, m] - fresh_ref[r - 1, m])
                tend = tend + u * (ue - uw) + v * (un - us)
                new = (1.0 - 4.0 * DT * VISC) * u - (0.5 * DT) * tend + coriolis * v
                target[1, r, m] = (new + (DT * VISC) * ((ue + uw) + (un + us))) * ocean
                fresh = fresh_ref[r, m]
                target[0, r, m] = fresh
                ve, vw = source[2, r + 1, m], source[2, r - 1, m]
                vn, vs = north(v), south(v)
                tend = GRAV * (north(fresh) - south(fresh)) + u * (ve - vw) + v * (vn - vs)
                new = (1.0 - 4.0 * DT * VISC) * v - (0.5 * DT) * tend - coriolis * u
                target[2, r, m] = (new + (DT * VISC) * ((ve + vw) + (vn + vs))) * ocean
            return carry

        lax.fori_loop(low + 2, rows - low - 2, flow_row, 0)
    source = target

    lane = lax.broadcasted_iota(jnp.int32, (members, LANES), 1)

    def pick(o, found):
        cell = cells[0, o]
        row = cell // columns
        column = cell % columns
        start = pl.multiple_of((column // LANES) * LANES, LANES)
        block = source[0, HALO + row, :, pl.ds(start, LANES)]
        turned = pltpu.roll(block, (o - column % LANES + LANES) % LANES, 1)
        return jnp.where(lane == o, turned, found)

    picks = lax.fori_loop(0, LANES, pick, jnp.zeros((members, LANES), jnp.float32), unroll=8)
    per_row = columns // LANES
    spare = members // 3
    for f in range(3):
        part = picks[f * spare : (f + 1) * spare]
        for r in range(rows_here):
            for c in range(per_row):
                d = r * per_row + c
                out_ref[d, f * GROUP : f * GROUP + members, :] = source[
                    f, HALO + r, :, c * LANES : (c + 1) * LANES
                ]
                out_ref[d, f * GROUP + members : (f + 1) * GROUP, :] = part


def forecast(cells, wide, coriolis, members, blocks):
    rows, _, columns = wide.shape
    vmem = pl.BlockSpec(memory_space=pltpu.VMEM)
    return pl.pallas_call(
        forecast_kernel,
        out_shape=jax.ShapeDtypeStruct((blocks, 3 * GROUP, LANES), jnp.float32),
        in_specs=[pl.BlockSpec(memory_space=pltpu.SMEM), vmem, vmem],
        out_specs=vmem,
        scratch_shapes=[
            pltpu.VMEM((3, rows, members, columns), jnp.float32),
            pltpu.VMEM((3, rows, members, columns), jnp.float32),
            pltpu.VMEM((rows, members, columns), jnp.float32),
        ],
        compiler_params=room(16),
        name="forecast",
    )(cells, wide, coriolis)


def gram_kernel(own, gathered_ref, value_ref, error_ref, out_ref, picks_ref, stack_ref):
    devices = gathered_ref.shape[0]
    members = 12
    spare = members // 3
    for d in range(devices):
        for f in range(3):
            at = d * members + f * spare
            picks_ref[at : at + spare, :] = gathered_ref[
                d, f * GROUP + members : (f + 1) * GROUP, :
            ]
    picks = picks_ref[...]
    hmean = jnp.mean(picks, axis=0, keepdims=True)
    scaled = (picks - hmean) / error_ref[...]
    misfit = (value_ref[...] - hmean) / error_ref[...]
    scaled_halves = halves(scaled)
    gram = product(scaled_halves, scaled_halves, ((1,), (1,)))
    drive = product(
        halves(jnp.broadcast_to(misfit, (8, LANES))), scaled_halves, ((1,), (1,))
    )
    n = LANES
    row = lax.broadcasted_iota(jnp.int32, (n, n), 0)
    column = lax.broadcasted_iota(jnp.int32, (n, n), 1)
    middle = gram[n : 2 * n, n : 2 * n]
    stack_ref[0:n] = gram[0:n, n : 2 * n]
    stack_ref[n : 2 * n] = gram[0:n, 2 * n :]
    stack_ref[2 * n : 3 * n] = gram[n : 2 * n, 2 * n :]
    stack_ref[3 * n : 4 * n] = jnp.where(row <= column, gram[0:n, 0:n], middle)
    stack_ref[4 * n : 5 * n] = gram[2 * n :, 2 * n :]
    stack_ref[5 * n :] = jnp.zeros((n, n), jnp.float32)
    diagonal = jnp.sum(jnp.where(row == column, middle, 0.0), axis=0, keepdims=True)
    stack_ref[5 * n : 5 * n + 1] = diagonal
    for k in range(3):
        stack_ref[5 * n + 8 * (k + 1) : 5 * n + 8 * (k + 2)] = drive[:, k * n : (k + 1) * n]
    size = out_ref.shape[1]
    piece = stack_ref[pl.ds(pl.multiple_of(own[0] * size, 8), size), :]
    out_ref[...] = jnp.broadcast_to(piece[None], out_ref.shape)


def gram_piece(own, gathered, value, error, slabs):
    devices = gathered.shape[0]
    ens = 3 * LANES
    size = 6 * LANES // devices
    vmem = pl.BlockSpec(memory_space=pltpu.VMEM)
    return pl.pallas_call(
        gram_kernel,
        out_shape=jax.ShapeDtypeStruct((slabs, size, LANES), jnp.float32),
        in_specs=[pl.BlockSpec(memory_space=pltpu.SMEM), vmem, vmem, vmem],
        out_specs=vmem,
        scratch_shapes=[
            pltpu.VMEM((ens, LANES), jnp.float32),
            pltpu.VMEM((6 * LANES, LANES), jnp.float32),
        ],
        compiler_params=room(8),
        name="gram",
    )(own, gathered, value, error)


def total_kernel(parts_ref, out_ref):
    total = jnp.sum(parts_ref[...], axis=0, keepdims=True)
    out_ref[...] = jnp.broadcast_to(total, out_ref.shape)


def total_piece(parts, devices):
    vmem = pl.BlockSpec(memory_space=pltpu.VMEM)
    return pl.pallas_call(
        total_kernel,
        out_shape=jax.ShapeDtypeStruct((devices, *parts.shape[1:]), jnp.float32),
        in_specs=[vmem],
        out_specs=vmem,
        compiler_params=room(8),
        name="total",
    )(parts)


def analysis_kernel(stack_ref, gathered_ref, out_ref, gram_ref, field_ref):
    n = LANES
    ens = 3 * n
    devices = gathered_ref.shape[0]
    members = ens // devices
    row = lax.broadcasted_iota(jnp.int32, (n, n), 0)
    column = lax.broadcasted_iota(jnp.int32, (n, n), 1)

    def block(k):
        return stack_ref[k * n : (k + 1) * n]

    for k, (i, j) in enumerate(((0, 1), (0, 2), (1, 2))):
        gram_ref[i * n : (i + 1) * n, j * n : (j + 1) * n] = block(k)
        gram_ref[j * n : (j + 1) * n, i * n : (i + 1) * n] = block(k).T
    both = block(3)
    upper = jnp.where(row < column, both, 0.0)
    gram_ref[0:n, 0:n] = upper + upper.T + jnp.where(row == column, both, 0.0)
    lower = jnp.where(row > column, both, 0.0)
    middle = jnp.where(row == column, stack_ref[5 * n : 5 * n + 1], 0.0)
    gram_ref[n : 2 * n, n : 2 * n] = lower + lower.T + middle
    gram_ref[2 * n :, 2 * n :] = block(4)
    drive = jnp.concatenate(
        [stack_ref[5 * n + 8 * (k + 1) : 5 * n + 8 * (k + 1) + 1] for k in range(3)], axis=1
    )

    same = lax.broadcasted_iota(jnp.int32, (ens, ens), 0) == lax.broadcasted_iota(
        jnp.int32, (ens, ens), 1
    )
    identity = jnp.where(same, 1.0, 0.0)
    system = identity + gram_ref[...] * (1.0 / (ens - 1))
    norm_scale = jnp.sqrt(jnp.sum(system * system, keepdims=True))
    iterate = system / norm_scale
    inverse = 1.5 * identity - 0.5 * iterate
    iterate = product(halves(iterate), halves(inverse))
    for sweep in range(1, NS_ITERS):
        iterate_halves = halves(iterate)
        inverse_halves = halves(inverse)
        factor_halves = halves(1.5 * identity - 0.5 * product(inverse_halves, iterate_halves))
        inverse = product(inverse_halves, factor_halves)
        if sweep + 1 < NS_ITERS:
            iterate = product(iterate_halves, factor_halves)
    weights = inverse / jnp.sqrt(norm_scale)
    pulled = jnp.sum(weights * drive, axis=1, keepdims=True)
    mean_weight = jnp.sum(weights * pulled, axis=0, keepdims=True) * (1.0 / (ens - 1))
    combined = halves(weights + mean_weight)

    for f in range(3):
        for d in range(devices):
            field_ref[f, d * members : (d + 1) * members, :] = gathered_ref[
                d, f * GROUP : f * GROUP + members, :
            ]
    for f in range(3):
        field = field_ref[f]
        center = jnp.mean(field, axis=0, keepdims=True)
        field_ref[f] = center + product(combined, halves(field - center))
    for f in range(3):
        for d in range(devices):
            out_ref[d, f * members : (f + 1) * members, :] = field_ref[
                f, d * members : (d + 1) * members, :
            ]


def analysis(stack, gathered):
    devices = gathered.shape[0]
    ens = 3 * LANES
    vmem = pl.BlockSpec(memory_space=pltpu.VMEM)
    return pl.pallas_call(
        analysis_kernel,
        out_shape=jax.ShapeDtypeStruct((devices, 3 * ens // devices, LANES), jnp.float32),
        in_specs=[vmem, vmem],
        out_specs=vmem,
        scratch_shapes=[
            pltpu.VMEM((ens, ens), jnp.float32),
            pltpu.VMEM((3, ens, LANES), jnp.float32),
        ],
        compiler_params=room(16),
        name="analysis",
    )(stack, gathered)


def local(ensemble, sea_depth, ocean_mask, observed_cells, observed_values, observed_error):
    local_members, fields, rows_here, columns = ensemble.shape
    devices = lax.axis_size(MEM)
    slabs = lax.axis_size("space")
    coriolis = 0.05 + 0.1 * jnp.arange(columns, dtype=jnp.float32)[None] / columns
    still = jnp.stack([sea_depth, ocean_mask.astype(jnp.float32)], axis=1)
    moving = ensemble.transpose(2, 1, 0, 3).reshape(rows_here, fields * local_members, columns)
    planes = jnp.concatenate([moving, still], axis=1)
    edge = HALO - rows_here
    before = lax.ppermute(planes, "space", ring("space", 1))
    after = lax.ppermute(planes, "space", ring("space", -1))
    far_before = lax.ppermute(planes[rows_here - edge :], "space", ring("space", 2))
    far_after = lax.ppermute(planes[:edge], "space", ring("space", -2))
    wide = jnp.concatenate([far_before, before, planes, after, far_after], axis=0)
    sent = forecast(observed_cells, wide, coriolis, local_members, devices)
    gathered = lax.all_to_all(sent, MEM, 0, 0, tiled=True)
    own = lax.axis_index(MEM).astype(jnp.int32).reshape(1)
    parts = gram_piece(own, gathered, observed_values, observed_error, slabs)
    parts = lax.all_to_all(parts, "space", 0, 0, tiled=True)
    pieces = lax.all_to_all(total_piece(parts, devices), MEM, 0, 0, tiled=True)
    result = analysis(pieces.reshape(-1, LANES), gathered)
    returned = lax.all_to_all(result, MEM, 0, 0, tiled=True)
    returned = returned.reshape(rows_here, columns // LANES, fields, local_members, LANES)
    return returned.transpose(3, 2, 0, 1, 4).reshape(ensemble.shape)


def solution(mesh):
    finer = Mesh(mesh.devices.reshape(8, 4, mesh.shape["space"]), ("mem_0", "mem_1", "space"))
    return jax.shard_map(
        local,
        mesh=finer,
        in_specs=(
            P(MEM, None, "space", None),
            P("space", None),
            P("space", None),
            P("space", None),
            P("space", None),
            P("space", None),
        ),
        out_specs=P(MEM, None, "space", None),
        check_vma=False,
    )
```

```python
import functools

import jax
import jax.numpy as jnp
from jax import lax
from jax.experimental import pallas as pl
from jax.experimental.pallas import tpu as pltpu
from jax.sharding import Mesh
from jax.sharding import PartitionSpec as P

STEPS = 3
NS_ITERS = 6
MEM = ("mem_0", "mem_1")

GRAV = 1.0
DT = 0.3
VISC = 0.1

LANES = 128
GROUP = 16
HALO = 2 * STEPS


def ring(axis, turn):
    count = lax.axis_size(axis)
    return [(i, (i + turn) % count) for i in range(count)]


def halves(x):
    top = x.astype(jnp.bfloat16)
    return top, (x - top.astype(jnp.float32)).astype(jnp.bfloat16)


def product(a, b, contract=((1,), (0,))):
    left = jnp.concatenate([a[0], a[0], a[1]], axis=contract[0][0])
    right = jnp.concatenate([b[0], b[1], b[0]], axis=contract[1][0])
    return lax.dot_general(left, right, (contract, ((), ())), preferred_element_type=jnp.float32)


def room(mebibytes):
    return pltpu.CompilerParams(vmem_limit_bytes=mebibytes << 20)


def planes_kernel(state_hbm, depth_hbm, ocean_hbm, out_ref, state_ref, depth_ref, ocean_ref, sems):
    members, fields, rows, columns = state_ref.shape
    copies = [
        pltpu.make_async_copy(source, target, sems.at[k])
        for k, (source, target) in enumerate(
            ((depth_hbm, depth_ref), (ocean_hbm, ocean_ref), (state_hbm, state_ref))
        )
    ]
    for copy in copies:
        copy.start()
    copies[0].wait()
    copies[1].wait()
    at = fields * members
    depth = depth_ref[...]
    ocean = ocean_ref[...].astype(jnp.float32)
    for r in range(rows):
        out_ref[r, at : at + 1, :] = depth[r : r + 1]
        out_ref[r, at + 1 : at + 2, :] = ocean[r : r + 1]
        out_ref[r, at + 2 : at + 4, :] = jnp.zeros((2, columns), jnp.float32)
    copies[2].wait()
    for f in range(fields):
        for m in range(members):
            at = f * members + m
            plane = state_ref[m, f]
            for r in range(rows):
                out_ref[r, at : at + 1, :] = plane[r : r + 1]


def planes_of(state, depth, ocean):
    members, fields, rows, columns = state.shape
    return pl.pallas_call(
        planes_kernel,
        out_shape=jax.ShapeDtypeStruct((rows, fields * members + 4, columns), jnp.float32),
        in_specs=[pl.BlockSpec(memory_space=pltpu.HBM)] * 3,
        out_specs=pl.BlockSpec(memory_space=pltpu.VMEM),
        scratch_shapes=[
            pltpu.VMEM(state.shape, jnp.float32),
            pltpu.VMEM(depth.shape, jnp.float32),
            pltpu.VMEM(ocean.shape, jnp.int32),
            pltpu.SemaphoreType.DMA((3,)),
        ],
        compiler_params=room(8),
        name="planes",
    )(*(pltpu.with_memory_space_constraint(x, pltpu.HBM) for x in (state, depth, ocean)))


def forecast_kernel(
    places,
    far_before_ref,
    before_ref,
    own_ref,
    after_ref,
    far_after_ref,
    coriolis_ref,
    out_ref,
    a_ref,
    b_ref,
    fresh_ref,
    still_ref,
):
    _, rows, members, columns = a_ref.shape
    rows_here = own_ref.shape[0]
    coriolis = coriolis_ref[...] * DT
    parts = [slice(at, min(at + 8, members)) for at in range(0, members, 8)]

    def north(x):
        return pltpu.roll(x, columns - 1, 1)

    def south(x):
        return pltpu.roll(x, 1, 1)

    at = 0
    for piece in (far_before_ref, before_ref, own_ref, after_ref, far_after_ref):

        def unpack(r, carry, piece=piece, at=at):
            for f in range(3):
                b_ref[f, at + r] = piece[r, f * members : (f + 1) * members, :]
            still_ref[at + r] = piece[r, 3 * members : 3 * members + 2, :]
            return carry

        lax.fori_loop(0, piece.shape[0], unpack, 0)
        at += piece.shape[0]

    for step in range(STEPS):
        source, target = (b_ref, a_ref) if step % 2 == 0 else (a_ref, b_ref)
        low = 2 * step

        def height_row(r, carry, source=source):
            depth_above = still_ref[r + 1, 0:1]
            depth_below = still_ref[r - 1, 0:1]
            depth = still_ref[r, 0:1]
            for m in parts:
                above = (depth_above + source[0, r + 1, m]) * source[1, r + 1, m]
                below = (depth_below + source[0, r - 1, m]) * source[1, r - 1, m]
                height = source[0, r, m]
                across = (depth + height) * source[2, r, m]
                fresh_ref[r, m] = height - (0.5 * DT) * (
                    (above - below) + (north(across) - south(across))
                )
            return carry

        lax.fori_loop(low + 1, rows - low - 1, height_row, 0)

        def flow_row(r, carry, source=source, target=target):
            ocean = still_ref[r, 1:2]
            for m in parts:
                u, v = source[1, r, m], source[2, r, m]
                ue, uw = source[1, r + 1, m], source[1, r - 1, m]
                un, us = north(u), south(u)
                tend = GRAV * (fresh_ref[r + 1, m] - fresh_ref[r - 1, m])
                tend = tend + u * (ue - uw) + v * (un - us)
                new = (1.0 - 4.0 * DT * VISC) * u - (0.5 * DT) * tend + coriolis * v
                target[1, r, m] = (new + (DT * VISC) * ((ue + uw) + (un + us))) * ocean
                fresh = fresh_ref[r, m]
                target[0, r, m] = fresh
                ve, vw = source[2, r + 1, m], source[2, r - 1, m]
                vn, vs = north(v), south(v)
                tend = GRAV * (north(fresh) - south(fresh)) + u * (ve - vw) + v * (vn - vs)
                new = (1.0 - 4.0 * DT * VISC) * v - (0.5 * DT) * tend - coriolis * u
                target[2, r, m] = (new + (DT * VISC) * ((ve + vw) + (vn + vs))) * ocean
            return carry

        lax.fori_loop(low + 2, rows - low - 2, flow_row, 0)
    source = target

    lane = lax.broadcasted_iota(jnp.int32, (members, LANES), 1)

    def pick(o, found):
        start = pl.multiple_of(places[1, o], LANES)
        block = source[0, HALO + places[0, o], :, pl.ds(start, LANES)]
        return jnp.where(lane == o, pltpu.roll(block, places[2, o], 1), found)

    picks = lax.fori_loop(0, LANES, pick, jnp.zeros((members, LANES), jnp.float32), unroll=8)
    per_row = columns // LANES
    spare = members // 3
    for f in range(3):
        part = picks[f * spare : (f + 1) * spare]
        for r in range(rows_here):
            for c in range(per_row):
                d = r * per_row + c
                out_ref[d, f * GROUP : f * GROUP + members, :] = source[
                    f, HALO + r, :, c * LANES : (c + 1) * LANES
                ]
                out_ref[d, f * GROUP + members : (f + 1) * GROUP, :] = part


def forecast(places, pieces, coriolis, members, blocks):
    columns = pieces[0].shape[2]
    rows = sum(piece.shape[0] for piece in pieces)
    vmem = pl.BlockSpec(memory_space=pltpu.VMEM)
    return pl.pallas_call(
        forecast_kernel,
        out_shape=jax.ShapeDtypeStruct((blocks, 3 * GROUP, LANES), jnp.float32),
        in_specs=[pl.BlockSpec(memory_space=pltpu.SMEM)] + [vmem] * (len(pieces) + 1),
        out_specs=vmem,
        scratch_shapes=[
            pltpu.VMEM((3, rows, members, columns), jnp.float32),
            pltpu.VMEM((3, rows, members, columns), jnp.float32),
            pltpu.VMEM((rows, members, columns), jnp.float32),
            pltpu.VMEM((rows, 2, columns), jnp.float32),
        ],
        compiler_params=room(20),
        name="forecast",
    )(places, *pieces, coriolis)


def gram_kernel(own, gathered_ref, value_ref, error_ref, out_ref, picks_ref, stack_ref):
    devices = gathered_ref.shape[0]
    members = 12
    spare = members // 3
    for d in range(devices):
        for f in range(3):
            at = d * members + f * spare
            picks_ref[at : at + spare, :] = gathered_ref[
                d, f * GROUP + members : (f + 1) * GROUP, :
            ]
    picks = picks_ref[...]
    hmean = jnp.mean(picks, axis=0, keepdims=True)
    scaled = (picks - hmean) / error_ref[...]
    misfit = (value_ref[...] - hmean) / error_ref[...]
    scaled_halves = halves(scaled)
    gram = product(scaled_halves, scaled_halves, ((1,), (1,)))
    drive = product(
        halves(jnp.broadcast_to(misfit, (8, LANES))), scaled_halves, ((1,), (1,))
    )
    n = LANES
    row = lax.broadcasted_iota(jnp.int32, (n, n), 0)
    column = lax.broadcasted_iota(jnp.int32, (n, n), 1)
    middle = gram[n : 2 * n, n : 2 * n]
    stack_ref[0:n] = gram[0:n, n : 2 * n]
    stack_ref[n : 2 * n] = gram[0:n, 2 * n :]
    stack_ref[2 * n : 3 * n] = gram[n : 2 * n, 2 * n :]
    stack_ref[3 * n : 4 * n] = jnp.where(row <= column, gram[0:n, 0:n], middle)
    stack_ref[4 * n : 5 * n] = gram[2 * n :, 2 * n :]
    stack_ref[5 * n :] = jnp.zeros((n, n), jnp.float32)
    diagonal = jnp.sum(jnp.where(row == column, middle, 0.0), axis=0, keepdims=True)
    stack_ref[5 * n : 5 * n + 1] = diagonal
    for k in range(3):
        stack_ref[5 * n + 8 * (k + 1) : 5 * n + 8 * (k + 2)] = drive[:, k * n : (k + 1) * n]
    size = out_ref.shape[1]
    piece = stack_ref[pl.ds(pl.multiple_of(own[0] * size, 8), size), :]
    out_ref[...] = jnp.broadcast_to(piece[None], out_ref.shape)


def gram_piece(own, gathered, value, error, slabs):
    devices = gathered.shape[0]
    ens = 3 * LANES
    size = 6 * LANES // devices
    vmem = pl.BlockSpec(memory_space=pltpu.VMEM)
    return pl.pallas_call(
        gram_kernel,
        out_shape=jax.ShapeDtypeStruct((slabs, size, LANES), jnp.float32),
        in_specs=[pl.BlockSpec(memory_space=pltpu.SMEM), vmem, vmem, vmem],
        out_specs=vmem,
        scratch_shapes=[
            pltpu.VMEM((ens, LANES), jnp.float32),
            pltpu.VMEM((6 * LANES, LANES), jnp.float32),
        ],
        compiler_params=room(8),
        name="gram",
    )(own, gathered, value, error)


def total_kernel(parts_ref, out_ref):
    total = jnp.sum(parts_ref[...], axis=0, keepdims=True)
    out_ref[...] = jnp.broadcast_to(total, out_ref.shape)


def total_piece(parts, devices):
    vmem = pl.BlockSpec(memory_space=pltpu.VMEM)
    return pl.pallas_call(
        total_kernel,
        out_shape=jax.ShapeDtypeStruct((devices, *parts.shape[1:]), jnp.float32),
        in_specs=[vmem],
        out_specs=vmem,
        compiler_params=room(8),
        name="total",
    )(parts)


def analysis_kernel(stack_ref, gathered_ref, out_ref, gram_ref, field_ref):
    n = LANES
    ens = 3 * n
    devices = gathered_ref.shape[0]
    members = ens // devices
    quads = members // 4
    row = lax.broadcasted_iota(jnp.int32, (n, n), 0)
    column = lax.broadcasted_iota(jnp.int32, (n, n), 1)

    def block(k):
        return stack_ref[k * n : (k + 1) * n]

    for k, (i, j) in enumerate(((0, 1), (0, 2), (1, 2))):
        gram_ref[i * n : (i + 1) * n, j * n : (j + 1) * n] = block(k)
        gram_ref[j * n : (j + 1) * n, i * n : (i + 1) * n] = block(k).T
    both = block(3)
    upper = jnp.where(row < column, both, 0.0)
    gram_ref[0:n, 0:n] = upper + upper.T + jnp.where(row == column, both, 0.0)
    lower = jnp.where(row > column, both, 0.0)
    middle = jnp.where(row == column, stack_ref[5 * n : 5 * n + 1], 0.0)
    gram_ref[n : 2 * n, n : 2 * n] = lower + lower.T + middle
    gram_ref[2 * n :, 2 * n :] = block(4)
    drive = jnp.concatenate(
        [stack_ref[5 * n + 8 * (k + 1) : 5 * n + 8 * (k + 1) + 1] for k in range(3)], axis=1
    )

    same = lax.broadcasted_iota(jnp.int32, (ens, ens), 0) == lax.broadcasted_iota(
        jnp.int32, (ens, ens), 1
    )
    identity = jnp.where(same, 1.0, 0.0)
    system = identity + gram_ref[...] * (1.0 / (ens - 1))
    norm_scale = jnp.sqrt(jnp.sum(system * system, keepdims=True))
    whole = system / norm_scale
    inverse = None
    for pair in range(NS_ITERS // 2):
        whole_halves = halves(whole)
        square = product(whole_halves, whole_halves)
        inner = 1.6875 * identity - 0.5625 * whole + 0.0625 * square
        quartic = product(halves(inner), halves(square)) + (2.25 * identity - 2.4375 * whole)
        quartic_halves = halves(quartic)
        inverse = quartic if pair == 0 else product(halves(inverse), quartic_halves)
        if 2 * pair + 2 < NS_ITERS:
            growth = product(quartic_halves, quartic_halves)
            whole = product(whole_halves, halves(growth))
    weights = inverse / jnp.sqrt(norm_scale)
    pulled = jnp.sum(weights * drive, axis=1, keepdims=True)
    mean_weight = jnp.sum(weights * pulled, axis=0, keepdims=True) * (1.0 / (ens - 1))
    combined = halves(weights + mean_weight)

    for f in range(3):
        for d in range(devices):
            field_ref[f, d * members : (d + 1) * members, :] = gathered_ref[
                d, f * GROUP : f * GROUP + members, :
            ]
    for f in range(3):
        field = field_ref[f]
        center = jnp.mean(field, axis=0, keepdims=True)
        field_ref[f] = center + product(combined, halves(field - center))
    for f in range(3):
        for d in range(devices):
            part = field_ref[f, d * members : (d + 1) * members, :]
            out_ref[d, f * quads : (f + 1) * quads] = part.reshape(quads, 4, n)


def analysis(stack, gathered):
    devices = gathered.shape[0]
    ens = 3 * LANES
    vmem = pl.BlockSpec(memory_space=pltpu.VMEM)
    return pl.pallas_call(
        analysis_kernel,
        out_shape=jax.ShapeDtypeStruct((devices, 3 * ens // devices // 4, 4, LANES), jnp.float32),
        in_specs=[vmem, vmem],
        out_specs=vmem,
        scratch_shapes=[
            pltpu.VMEM((ens, ens), jnp.float32),
            pltpu.VMEM((3, ens, LANES), jnp.float32),
        ],
        compiler_params=room(16),
        name="analysis",
    )(stack, gathered)


def local(ensemble, sea_depth, ocean_mask, observed_cells, observed_values, observed_error):
    local_members, fields, rows_here, columns = ensemble.shape
    devices = lax.axis_size(MEM)
    slabs = lax.axis_size("space")
    coriolis = 0.05 + 0.1 * jnp.arange(columns, dtype=jnp.float32)[None] / columns
    cells = observed_cells[0]
    places = jnp.stack(
        [
            cells // columns,
            cells % columns // LANES * LANES,
            (jnp.arange(LANES, dtype=jnp.int32) - cells) % LANES,
        ]
    )
    own = lax.axis_index(MEM).astype(jnp.int32).reshape(1)
    planes = planes_of(ensemble, sea_depth, ocean_mask)
    edge = HALO - rows_here
    before = lax.ppermute(planes, "space", ring("space", 1))
    after = lax.ppermute(planes, "space", ring("space", -1))
    far_before = lax.ppermute(planes[rows_here - edge :], "space", ring("space", 2))
    far_after = lax.ppermute(planes[:edge], "space", ring("space", -2))
    pieces = (far_before, before, planes, after, far_after)
    sent = forecast(places, pieces, coriolis, local_members, devices)
    gathered = lax.all_to_all(sent, MEM, 0, 0, tiled=True)
    parts = gram_piece(own, gathered, observed_values, observed_error, slabs)
    parts = lax.all_to_all(parts, "space", 0, 0, tiled=True)
    pieces = lax.all_to_all(total_piece(parts, devices), MEM, 0, 0, tiled=True)
    result = analysis(pieces.reshape(-1, LANES), gathered)
    returned = lax.all_to_all(result, MEM, 0, 0, tiled=True)
    returned = returned.reshape(rows_here, columns // LANES, fields, local_members, LANES)
    return returned.transpose(3, 2, 0, 1, 4).reshape(ensemble.shape)


def solution(mesh):
    finer = Mesh(mesh.devices.reshape(8, 4, mesh.shape["space"]), ("mem_0", "mem_1", "space"))
    return jax.shard_map(
        local,
        mesh=finer,
        in_specs=(
            P(MEM, None, "space", None),
            P("space", None),
            P("space", None),
            P("space", None),
            P("space", None),
            P("space", None),
        ),
        out_specs=P(MEM, None, "space", None),
        check_vma=False,
    )
```

```python
import functools

import jax
import jax.numpy as jnp
from jax import lax
from jax.experimental import pallas as pl
from jax.experimental.pallas import tpu as pltpu
from jax.sharding import Mesh
from jax.sharding import PartitionSpec as P

STEPS = 3
NS_ITERS = 6
MEM = ("mem_0", "mem_1")

GRAV = 1.0
DT = 0.3
VISC = 0.1

LANES = 128
GROUP = 16
HALO = 2 * STEPS


def ring(axis, turn):
    count = lax.axis_size(axis)
    return [(i, (i + turn) % count) for i in range(count)]


def halves(x):
    top = x.astype(jnp.bfloat16)
    return top, (x - top.astype(jnp.float32)).astype(jnp.bfloat16)


def product(a, b, contract=((1,), (0,))):
    left = jnp.concatenate([a[0], a[0], a[1]], axis=contract[0][0])
    right = jnp.concatenate([b[0], b[1], b[0]], axis=contract[1][0])
    return lax.dot_general(left, right, (contract, ((), ())), preferred_element_type=jnp.float32)


def room(mebibytes):
    return pltpu.CompilerParams(vmem_limit_bytes=mebibytes << 20)


def planes_kernel(state_hbm, depth_hbm, ocean_hbm, out_ref, state_ref, depth_ref, ocean_ref, sems):
    members, fields, rows, columns = state_ref.shape
    copies = [
        pltpu.make_async_copy(source, target, sems.at[k])
        for k, (source, target) in enumerate(
            ((depth_hbm, depth_ref), (ocean_hbm, ocean_ref), (state_hbm, state_ref))
        )
    ]
    for copy in copies:
        copy.start()
    copies[0].wait()
    copies[1].wait()
    at = fields * members
    depth = depth_ref[...]
    ocean = ocean_ref[...].astype(jnp.float32)
    for r in range(rows):
        out_ref[r, at : at + 1, :] = depth[r : r + 1]
        out_ref[r, at + 1 : at + 2, :] = ocean[r : r + 1]
        out_ref[r, at + 2 : at + 4, :] = jnp.zeros((2, columns), jnp.float32)
    copies[2].wait()
    for f in range(fields):
        for m in range(members):
            at = f * members + m
            plane = state_ref[m, f]
            for r in range(rows):
                out_ref[r, at : at + 1, :] = plane[r : r + 1]


def planes_of(state, depth, ocean):
    members, fields, rows, columns = state.shape
    return pl.pallas_call(
        planes_kernel,
        out_shape=jax.ShapeDtypeStruct((rows, fields * members + 4, columns), jnp.float32),
        in_specs=[pl.BlockSpec(memory_space=pltpu.HBM)] * 3,
        out_specs=pl.BlockSpec(memory_space=pltpu.VMEM),
        scratch_shapes=[
            pltpu.VMEM(state.shape, jnp.float32),
            pltpu.VMEM(depth.shape, jnp.float32),
            pltpu.VMEM(ocean.shape, jnp.int32),
            pltpu.SemaphoreType.DMA((3,)),
        ],
        compiler_params=room(8),
        name="planes",
    )(*(pltpu.with_memory_space_constraint(x, pltpu.HBM) for x in (state, depth, ocean)))


def north(x):
    return pltpu.roll(x, x.shape[1] - 1, 1)


def south(x):
    return pltpu.roll(x, 1, 1)


def sublane_parts(members):
    return [slice(at, min(at + 8, members)) for at in range(0, members, 8)]


def advance(source, target, still, fresh_ref, coriolis, first, last):
    parts = sublane_parts(source.shape[2])

    def height_row(r, carry):
        depth_above = still[r + 1, 0:1]
        depth_below = still[r - 1, 0:1]
        depth = still[r, 0:1]
        for m in parts:
            above = (depth_above + source[0, r + 1, m]) * source[1, r + 1, m]
            below = (depth_below + source[0, r - 1, m]) * source[1, r - 1, m]
            height = source[0, r, m]
            across = (depth + height) * source[2, r, m]
            fresh_ref[r, m] = height - (0.5 * DT) * (
                (above - below) + (north(across) - south(across))
            )
        return carry

    lax.fori_loop(first - 1, last + 2, height_row, 0)

    def flow_row(r, carry):
        ocean = still[r, 1:2]
        for m in parts:
            u, v = source[1, r, m], source[2, r, m]
            ue, uw = source[1, r + 1, m], source[1, r - 1, m]
            un, us = north(u), south(u)
            tend = GRAV * (fresh_ref[r + 1, m] - fresh_ref[r - 1, m])
            tend = tend + u * (ue - uw) + v * (un - us)
            new = (1.0 - 4.0 * DT * VISC) * u - (0.5 * DT) * tend + coriolis * v
            target[1, r, m] = (new + (DT * VISC) * ((ue + uw) + (un + us))) * ocean
            fresh = fresh_ref[r, m]
            target[0, r, m] = fresh
            ve, vw = source[2, r + 1, m], source[2, r - 1, m]
            vn, vs = north(v), south(v)
            tend = GRAV * (north(fresh) - south(fresh)) + u * (ve - vw) + v * (vn - vs)
            new = (1.0 - 4.0 * DT * VISC) * v - (0.5 * DT) * tend - coriolis * u
            target[2, r, m] = (new + (DT * VISC) * ((ve + vw) + (vn + vs))) * ocean
        return carry

    lax.fori_loop(first, last + 1, flow_row, 0)


def unpack(piece, count, at, state_ref, still_ref):
    members = state_ref.shape[2]

    def row(r, carry):
        for f in range(3):
            state_ref[f, at + r] = piece[r, f * members : (f + 1) * members, :]
        still_ref[at + r] = piece[r, 3 * members : 3 * members + 2, :]
        return carry

    lax.fori_loop(0, count, row, 0)


def inner_kernel(
    before_ref, own_ref, after_ref, coriolis_ref, one_ref, two_ref, raw_ref, a_ref, b_ref,
    fresh_ref, still_ref,
):
    coriolis = coriolis_ref[...] * DT
    for at, piece in ((2, before_ref), (6, own_ref), (10, after_ref)):
        unpack(piece, 4, at, raw_ref, still_ref)
    advance(raw_ref, a_ref, still_ref, fresh_ref, coriolis, 4, 11)
    advance(a_ref, b_ref, still_ref, fresh_ref, coriolis, 6, 9)
    for f in range(3):
        for r in range(8):
            one_ref[f, r] = a_ref[f, 4 + r]
        for r in range(4):
            two_ref[f, r] = b_ref[f, 6 + r]


def outer_kernel(
    places,
    far_before_ref,
    before_ref,
    own_ref,
    after_ref,
    far_after_ref,
    one_ref,
    two_ref,
    coriolis_ref,
    out_ref,
    raw_ref,
    a_ref,
    b_ref,
    fresh_ref,
    still_ref,
):
    members, columns = raw_ref.shape[2:]
    rows_here = own_ref.shape[0]
    coriolis = coriolis_ref[...] * DT
    for at, piece in ((0, far_before_ref), (2, before_ref), (10, after_ref), (14, far_after_ref)):
        unpack(piece, piece.shape[0], at, raw_ref, still_ref)
    for r in range(rows_here):
        still_ref[6 + r] = own_ref[r, 3 * members : 3 * members + 2, :]
    for f in range(3):
        for r in range(8):
            a_ref[f, 4 + r] = one_ref[f, r]
        for r in range(4):
            b_ref[f, 6 + r] = two_ref[f, r]
    advance(raw_ref, a_ref, still_ref, fresh_ref, coriolis, 2, 3)
    advance(raw_ref, a_ref, still_ref, fresh_ref, coriolis, 12, 13)
    advance(a_ref, b_ref, still_ref, fresh_ref, coriolis, 4, 5)
    advance(a_ref, b_ref, still_ref, fresh_ref, coriolis, 10, 11)
    advance(b_ref, raw_ref, still_ref, fresh_ref, coriolis, 6, 9)
    source = raw_ref
    lane = lax.broadcasted_iota(jnp.int32, (members, LANES), 1)

    def pick(o, found):
        start = pl.multiple_of(places[1, o], LANES)
        block = source[0, HALO + places[0, o], :, pl.ds(start, LANES)]
        return jnp.where(lane == o, pltpu.roll(block, places[2, o], 1), found)

    picks = lax.fori_loop(0, LANES, pick, jnp.zeros((members, LANES), jnp.float32), unroll=8)
    per_row = columns // LANES
    spare = members // 3
    for f in range(3):
        part = picks[f * spare : (f + 1) * spare]
        for r in range(rows_here):
            for c in range(per_row):
                d = r * per_row + c
                out_ref[d, f * GROUP : f * GROUP + members, :] = source[
                    f, HALO + r, :, c * LANES : (c + 1) * LANES
                ]
                out_ref[d, f * GROUP + members : (f + 1) * GROUP, :] = part


def frame(members, columns):
    rows = 2 * HALO + 4
    return [pltpu.VMEM((3, rows, members, columns), jnp.float32)] * 3 + [
        pltpu.VMEM((rows, members, columns), jnp.float32),
        pltpu.VMEM((rows, 2, columns), jnp.float32),
    ]


def inner_rows(near, coriolis, members):
    columns = near[0].shape[2]
    vmem = pl.BlockSpec(memory_space=pltpu.VMEM)
    return pl.pallas_call(
        inner_kernel,
        out_shape=tuple(
            jax.ShapeDtypeStruct((3, rows, members, columns), jnp.float32) for rows in (8, 4)
        ),
        in_specs=[vmem] * 4,
        out_specs=(vmem, vmem),
        scratch_shapes=frame(members, columns),
        compiler_params=room(20),
        name="inner",
    )(*near, coriolis)


def forecast(places, pieces, inner, coriolis, members, blocks):
    columns = pieces[0].shape[2]
    vmem = pl.BlockSpec(memory_space=pltpu.VMEM)
    return pl.pallas_call(
        outer_kernel,
        out_shape=jax.ShapeDtypeStruct((blocks, 3 * GROUP, LANES), jnp.float32),
        in_specs=[pl.BlockSpec(memory_space=pltpu.SMEM)] + [vmem] * 8,
        out_specs=vmem,
        scratch_shapes=frame(members, columns),
        compiler_params=room(20),
        name="outer",
    )(places, *pieces, *inner, coriolis)


def gram_kernel(own, gathered_ref, value_ref, error_ref, out_ref, picks_ref, stack_ref):
    devices = gathered_ref.shape[0]
    members = 12
    spare = members // 3
    for d in range(devices):
        for f in range(3):
            at = d * members + f * spare
            picks_ref[at : at + spare, :] = gathered_ref[
                d, f * GROUP + members : (f + 1) * GROUP, :
            ]
    picks = picks_ref[...]
    hmean = jnp.mean(picks, axis=0, keepdims=True)
    scaled = (picks - hmean) / error_ref[...]
    misfit = (value_ref[...] - hmean) / error_ref[...]
    scaled_halves = halves(scaled)
    gram = product(scaled_halves, scaled_halves, ((1,), (1,)))
    drive = product(
        halves(jnp.broadcast_to(misfit, (8, LANES))), scaled_halves, ((1,), (1,))
    )
    n = LANES
    row = lax.broadcasted_iota(jnp.int32, (n, n), 0)
    column = lax.broadcasted_iota(jnp.int32, (n, n), 1)
    middle = gram[n : 2 * n, n : 2 * n]
    diagonal = jnp.sum(jnp.where(row == column, middle, 0.0), axis=0, keepdims=True)
    last = gram[2 * n :, 2 * n :]
    vectors = [jnp.broadcast_to(diagonal, (8, n))]
    vectors += [drive[:, k * n : (k + 1) * n] for k in range(3)]
    for k, vector in enumerate(vectors):
        turned = pltpu.roll(vector, n // 2, 1)
        left = column < n // 2
        last = jnp.where((row == n - 8 + 2 * k) & left, vector[0:1], last)
        last = jnp.where((row == n - 7 + 2 * k) & left, turned[0:1], last)
    blocks = (
        gram[0:n, n : 2 * n],
        gram[0:n, 2 * n :],
        gram[n : 2 * n, 2 * n :],
        jnp.where(row <= column, gram[0:n, 0:n], middle),
        last,
    )
    quads = n // 4
    for k, block in enumerate(blocks):
        stack_ref[k * quads : (k + 1) * quads] = block.reshape(quads, 4, n)
    size = out_ref.shape[1]
    piece = stack_ref[pl.ds(own[0] * size, size)]
    out_ref[...] = jnp.broadcast_to(piece[None], out_ref.shape)


def gram_piece(own, gathered, value, error, slabs):
    devices = gathered.shape[0]
    ens = 3 * LANES
    size = 5 * LANES // 4 // devices
    vmem = pl.BlockSpec(memory_space=pltpu.VMEM)
    return pl.pallas_call(
        gram_kernel,
        out_shape=jax.ShapeDtypeStruct((slabs, size, 4, LANES), jnp.float32),
        in_specs=[pl.BlockSpec(memory_space=pltpu.SMEM), vmem, vmem, vmem],
        out_specs=vmem,
        scratch_shapes=[
            pltpu.VMEM((ens, LANES), jnp.float32),
            pltpu.VMEM((5 * LANES // 4, 4, LANES), jnp.float32),
        ],
        compiler_params=room(8),
        name="gram",
    )(own, gathered, value, error)


def total_kernel(parts_ref, out_ref):
    total = jnp.sum(parts_ref[...], axis=0, keepdims=True)
    out_ref[...] = jnp.broadcast_to(total, out_ref.shape)


def total_piece(parts, devices):
    vmem = pl.BlockSpec(memory_space=pltpu.VMEM)
    return pl.pallas_call(
        total_kernel,
        out_shape=jax.ShapeDtypeStruct((devices, *parts.shape[1:]), jnp.float32),
        in_specs=[vmem],
        out_specs=vmem,
        compiler_params=room(8),
        name="total",
    )(parts)


def analysis_kernel(stack_ref, gathered_ref, out_ref, gram_ref, field_ref):
    n = LANES
    ens = 3 * n
    devices = gathered_ref.shape[0]
    members = ens // devices
    quads = members // 4
    row = lax.broadcasted_iota(jnp.int32, (n, n), 0)
    column = lax.broadcasted_iota(jnp.int32, (n, n), 1)

    def block(k):
        return stack_ref[k * n // 4 : (k + 1) * n // 4].reshape(n, n)

    for k, (i, j) in enumerate(((0, 1), (0, 2), (1, 2))):
        gram_ref[i * n : (i + 1) * n, j * n : (j + 1) * n] = block(k)
        gram_ref[j * n : (j + 1) * n, i * n : (i + 1) * n] = block(k).T
    both = block(3)
    upper = jnp.where(row < column, both, 0.0)
    gram_ref[0:n, 0:n] = upper + upper.T + jnp.where(row == column, both, 0.0)
    lower = jnp.where(row > column, both, 0.0)
    last = block(4)
    tail = last[n - 8 :]
    turned = pltpu.roll(tail, n // 2, 1)
    left = column[0:1] < n // 2
    vectors = [
        jnp.where(left, tail[2 * k : 2 * k + 1], turned[2 * k + 1 : 2 * k + 2]) for k in range(4)
    ]
    middle = jnp.where(row == column, vectors[0], 0.0)
    gram_ref[n : 2 * n, n : 2 * n] = lower + lower.T + middle
    upper = jnp.where(row < column, last, 0.0)
    gram_ref[2 * n :, 2 * n :] = upper + upper.T + jnp.where(row == column, last, 0.0)
    drive = jnp.concatenate(vectors[1:], axis=1)

    same = lax.broadcasted_iota(jnp.int32, (ens, ens), 0) == lax.broadcasted_iota(
        jnp.int32, (ens, ens), 1
    )
    identity = jnp.where(same, 1.0, 0.0)
    system = identity + gram_ref[...] * (1.0 / (ens - 1))
    norm_scale = jnp.sqrt(jnp.sum(system * system, keepdims=True))
    whole = system / norm_scale
    inverse = None
    for pair in range(NS_ITERS // 2):
        whole_halves = halves(whole)
        square = product(whole_halves, whole_halves)
        inner = 1.6875 * identity - 0.5625 * whole + 0.0625 * square
        quartic = product(halves(inner), halves(square)) + (2.25 * identity - 2.4375 * whole)
        quartic_halves = halves(quartic)
        inverse = quartic if pair == 0 else product(halves(inverse), quartic_halves)
        if 2 * pair + 2 < NS_ITERS:
            growth = product(quartic_halves, quartic_halves)
            whole = product(whole_halves, halves(growth))
    weights = inverse / jnp.sqrt(norm_scale)
    pulled = jnp.sum(weights * drive, axis=1, keepdims=True)
    mean_weight = jnp.sum(weights * pulled, axis=0, keepdims=True) * (1.0 / (ens - 1))
    combined = halves(weights + mean_weight)

    for f in range(3):
        for d in range(devices):
            field_ref[f, d * members : (d + 1) * members, :] = gathered_ref[
                d, f * GROUP : f * GROUP + members, :
            ]
    for f in range(3):
        field = field_ref[f]
        center = jnp.mean(field, axis=0, keepdims=True)
        field_ref[f] = center + product(combined, halves(field - center))
    for f in range(3):
        for d in range(devices):
            part = field_ref[f, d * members : (d + 1) * members, :]
            out_ref[d, f * quads : (f + 1) * quads] = part.reshape(quads, 4, n)


def analysis(stack, gathered):
    devices = gathered.shape[0]
    ens = 3 * LANES
    vmem = pl.BlockSpec(memory_space=pltpu.VMEM)
    return pl.pallas_call(
        analysis_kernel,
        out_shape=jax.ShapeDtypeStruct((devices, 3 * ens // devices // 4, 4, LANES), jnp.float32),
        in_specs=[vmem, vmem],
        out_specs=vmem,
        scratch_shapes=[
            pltpu.VMEM((ens, ens), jnp.float32),
            pltpu.VMEM((3, ens, LANES), jnp.float32),
        ],
        compiler_params=room(16),
        name="analysis",
    )(stack, gathered)


def local(ensemble, sea_depth, ocean_mask, observed_cells, observed_values, observed_error):
    local_members, fields, rows_here, columns = ensemble.shape
    devices = lax.axis_size(MEM)
    slabs = lax.axis_size("space")
    coriolis = 0.05 + 0.1 * jnp.arange(columns, dtype=jnp.float32)[None] / columns
    cells = observed_cells[0]
    places = jnp.stack(
        [
            cells // columns,
            cells % columns // LANES * LANES,
            (jnp.arange(LANES, dtype=jnp.int32) - cells) % LANES,
        ]
    )
    own = lax.axis_index(MEM).astype(jnp.int32).reshape(1)
    planes = planes_of(ensemble, sea_depth, ocean_mask)
    edge = HALO - rows_here
    before = lax.ppermute(planes, "space", ring("space", 1))
    after = lax.ppermute(planes, "space", ring("space", -1))
    far_before = lax.ppermute(planes[rows_here - edge :], "space", ring("space", 2))
    far_after = lax.ppermute(planes[:edge], "space", ring("space", -2))
    inner = inner_rows((before, planes, after), coriolis, local_members)
    pieces = (far_before, before, planes, after, far_after)
    sent = forecast(places, pieces, inner, coriolis, local_members, devices)
    gathered = lax.all_to_all(sent, MEM, 0, 0, tiled=True)
    parts = gram_piece(own, gathered, observed_values, observed_error, slabs)
    parts = lax.all_to_all(parts, "space", 0, 0, tiled=True)
    pieces = lax.all_to_all(total_piece(parts, devices), MEM, 0, 0, tiled=True)
    result = analysis(pieces.reshape(-1, 4, LANES), gathered)
    returned = lax.all_to_all(result, MEM, 0, 0, tiled=True)
    returned = returned.reshape(rows_here, columns // LANES, fields, local_members, LANES)
    return returned.transpose(3, 2, 0, 1, 4).reshape(ensemble.shape)


def solution(mesh):
    finer = Mesh(mesh.devices.reshape(8, 4, mesh.shape["space"]), ("mem_0", "mem_1", "space"))
    return jax.shard_map(
        local,
        mesh=finer,
        in_specs=(
            P(MEM, None, "space", None),
            P("space", None),
            P("space", None),
            P("space", None),
            P("space", None),
            P("space", None),
        ),
        out_specs=P(MEM, None, "space", None),
        check_vma=False,
    )
```

```python
import functools

import jax
import jax.numpy as jnp
from jax import lax
from jax.experimental import pallas as pl
from jax.experimental.pallas import tpu as pltpu
from jax.sharding import Mesh
from jax.sharding import PartitionSpec as P

STEPS = 3
NS_ITERS = 6
MEM = ("mem_0", "mem_1")

GRAV = 1.0
DT = 0.3
VISC = 0.1

LANES = 128
GROUP = 16
HALO = 2 * STEPS


def ring(axis, turn):
    count = lax.axis_size(axis)
    return [(i, (i + turn) % count) for i in range(count)]


def halves(x):
    top = x.astype(jnp.bfloat16)
    return top, (x - top.astype(jnp.float32)).astype(jnp.bfloat16)


def product(a, b, contract=((1,), (0,))):
    left = jnp.concatenate([a[0], a[0], a[1]], axis=contract[0][0])
    right = jnp.concatenate([b[0], b[1], b[0]], axis=contract[1][0])
    return lax.dot_general(left, right, (contract, ((), ())), preferred_element_type=jnp.float32)


def room(mebibytes):
    return pltpu.CompilerParams(vmem_limit_bytes=mebibytes << 20)


def planes_kernel(state_hbm, depth_hbm, ocean_hbm, out_ref, state_ref, depth_ref, ocean_ref, sems):
    members, fields, rows, columns = state_ref.shape
    copies = [
        pltpu.make_async_copy(source, target, sems.at[k])
        for k, (source, target) in enumerate(
            ((depth_hbm, depth_ref), (ocean_hbm, ocean_ref), (state_hbm, state_ref))
        )
    ]
    for copy in copies:
        copy.start()
    copies[0].wait()
    copies[1].wait()
    at = fields * members
    depth = depth_ref[...]
    ocean = ocean_ref[...].astype(jnp.float32)
    for r in range(rows):
        out_ref[r, at : at + 1, :] = depth[r : r + 1]
        out_ref[r, at + 1 : at + 2, :] = ocean[r : r + 1]
        out_ref[r, at + 2 : at + 4, :] = jnp.zeros((2, columns), jnp.float32)
    copies[2].wait()
    for f in range(fields):
        for m in range(members):
            at = f * members + m
            plane = state_ref[m, f]
            for r in range(rows):
                out_ref[r, at : at + 1, :] = plane[r : r + 1]


def planes_of(state, depth, ocean):
    members, fields, rows, columns = state.shape
    return pl.pallas_call(
        planes_kernel,
        out_shape=jax.ShapeDtypeStruct((rows, fields * members + 4, columns), jnp.float32),
        in_specs=[pl.BlockSpec(memory_space=pltpu.HBM)] * 3,
        out_specs=pl.BlockSpec(memory_space=pltpu.VMEM),
        scratch_shapes=[
            pltpu.VMEM(state.shape, jnp.float32),
            pltpu.VMEM(depth.shape, jnp.float32),
            pltpu.VMEM(ocean.shape, jnp.int32),
            pltpu.SemaphoreType.DMA((3,)),
        ],
        compiler_params=room(8),
        name="planes",
    )(*(pltpu.with_memory_space_constraint(x, pltpu.HBM) for x in (state, depth, ocean)))


def north(x):
    return pltpu.roll(x, x.shape[1] - 1, 1)


def south(x):
    return pltpu.roll(x, 1, 1)


def sublane_parts(members):
    return [slice(at, min(at + 8, members)) for at in range(0, members, 8)]


def repeat(first, last, row, unroll):
    if unroll:
        for r in range(first, last):
            row(r, 0)
    else:
        lax.fori_loop(first, last, row, 0)


def rows_of(ref, inner=None, first=0, last=-1):
    def get(f, r, m):
        return (inner if inner is not None and first <= r <= last else ref)[f, r, m]

    return get


def advance(get, target, still, fresh_ref, coriolis, first, last, known=None, unroll=False):
    parts = sublane_parts(target.shape[2])

    def height_row(r, carry):
        depth_above = still[r + 1, 0:1]
        depth_below = still[r - 1, 0:1]
        depth = still[r, 0:1]
        for m in parts:
            above = (depth_above + get(0, r + 1, m)) * get(1, r + 1, m)
            below = (depth_below + get(0, r - 1, m)) * get(1, r - 1, m)
            height = get(0, r, m)
            across = (depth + height) * get(2, r, m)
            fresh_ref[r, m] = height - (0.5 * DT) * (
                (above - below) + (north(across) - south(across))
            )
        return carry

    low = first if known == first - 1 else first - 1
    high = last if known == last + 1 else last + 1
    repeat(low, high + 1, height_row, unroll)

    def flow_row(r, carry):
        ocean = still[r, 1:2]
        for m in parts:
            u, v = get(1, r, m), get(2, r, m)
            ue, uw = get(1, r + 1, m), get(1, r - 1, m)
            un, us = north(u), south(u)
            tend = GRAV * (fresh_ref[r + 1, m] - fresh_ref[r - 1, m])
            tend = tend + u * (ue - uw) + v * (un - us)
            new = (1.0 - 4.0 * DT * VISC) * u - (0.5 * DT) * tend + coriolis * v
            target[1, r, m] = (new + (DT * VISC) * ((ue + uw) + (un + us))) * ocean
            fresh = fresh_ref[r, m]
            target[0, r, m] = fresh
            ve, vw = get(2, r + 1, m), get(2, r - 1, m)
            vn, vs = north(v), south(v)
            tend = GRAV * (north(fresh) - south(fresh)) + u * (ve - vw) + v * (vn - vs)
            new = (1.0 - 4.0 * DT * VISC) * v - (0.5 * DT) * tend - coriolis * u
            target[2, r, m] = (new + (DT * VISC) * ((ve + vw) + (vn + vs))) * ocean
        return carry

    repeat(first, last + 1, flow_row, unroll)


def unpack(piece, count, at, state_ref, still_ref):
    members = state_ref.shape[2]

    def row(r, carry):
        for f in range(3):
            state_ref[f, at + r] = piece[r, f * members : (f + 1) * members, :]
        still_ref[at + r] = piece[r, 3 * members : 3 * members + 2, :]
        return carry

    lax.fori_loop(0, count, row, 0)


def inner_kernel(
    before_ref, own_ref, after_ref, coriolis_ref, a_ref, b_ref, raw_ref, fresh_ref, still_ref
):
    coriolis = coriolis_ref[...] * DT
    for at, piece in ((2, before_ref), (6, own_ref), (10, after_ref)):
        unpack(piece, 4, at, raw_ref, still_ref)
    advance(rows_of(raw_ref), a_ref, still_ref, fresh_ref, coriolis, 4, 11)
    advance(rows_of(a_ref), b_ref, still_ref, fresh_ref, coriolis, 6, 9)


def outer_kernel(
    places,
    far_before_ref,
    before_ref,
    own_ref,
    after_ref,
    far_after_ref,
    one_ref,
    two_ref,
    coriolis_ref,
    out_ref,
    a_ref,
    b_ref,
    raw_ref,
    fresh_ref,
    still_ref,
):
    members, columns = raw_ref.shape[2:]
    rows_here = own_ref.shape[0]
    coriolis = coriolis_ref[...] * DT
    for at, piece in ((0, far_before_ref), (2, before_ref), (10, after_ref), (14, far_after_ref)):
        unpack(piece, piece.shape[0], at, raw_ref, still_ref)
    for r in range(rows_here):
        still_ref[6 + r] = own_ref[r, 3 * members : 3 * members + 2, :]
    raw = rows_of(raw_ref)
    one = rows_of(a_ref, one_ref, 4, 11)
    two = rows_of(b_ref, two_ref, 6, 9)
    for r in (4, 11):
        fresh_ref[r] = one_ref[0, r]
    advance(raw, a_ref, still_ref, fresh_ref, coriolis, 2, 3, 4, True)
    advance(raw, a_ref, still_ref, fresh_ref, coriolis, 12, 13, 11, True)
    for r in (6, 9):
        fresh_ref[r] = two_ref[0, r]
    advance(one, b_ref, still_ref, fresh_ref, coriolis, 4, 5, 6, True)
    advance(one, b_ref, still_ref, fresh_ref, coriolis, 10, 11, 9, True)
    advance(two, raw_ref, still_ref, fresh_ref, coriolis, 6, 9, None, True)
    source = raw_ref
    lane = lax.broadcasted_iota(jnp.int32, (members, LANES), 1)

    def pick(o, found):
        start = pl.multiple_of(places[1, o], LANES)
        block = source[0, HALO + places[0, o], :, pl.ds(start, LANES)]
        return jnp.where(lane == o, pltpu.roll(block, places[2, o], 1), found)

    picks = lax.fori_loop(0, LANES, pick, jnp.zeros((members, LANES), jnp.float32), unroll=8)
    per_row = columns // LANES
    spare = members // 3
    for f in range(3):
        part = picks[f * spare : (f + 1) * spare]
        for r in range(rows_here):
            for c in range(per_row):
                d = r * per_row + c
                out_ref[d, f * GROUP : f * GROUP + members, :] = source[
                    f, HALO + r, :, c * LANES : (c + 1) * LANES
                ]
                out_ref[d, f * GROUP + members : (f + 1) * GROUP, :] = part


def frame(members, columns):
    rows = 2 * HALO + 4
    return [
        pltpu.VMEM((3, rows, members, columns), jnp.float32),
        pltpu.VMEM((rows, members, columns), jnp.float32),
        pltpu.VMEM((rows, 2, columns), jnp.float32),
    ]


def inner_rows(near, coriolis, members):
    columns = near[0].shape[2]
    vmem = pl.BlockSpec(memory_space=pltpu.VMEM)
    return pl.pallas_call(
        inner_kernel,
        out_shape=(
            jax.ShapeDtypeStruct((3, 2 * HALO + 4, members, columns), jnp.float32),
        ) * 2,
        in_specs=[vmem] * 4,
        out_specs=(vmem, vmem),
        scratch_shapes=frame(members, columns),
        compiler_params=room(20),
        name="inner",
    )(*near, coriolis)


def forecast(places, pieces, inner, coriolis, members, blocks):
    columns = pieces[0].shape[2]
    vmem = pl.BlockSpec(memory_space=pltpu.VMEM)
    return pl.pallas_call(
        outer_kernel,
        out_shape=jax.ShapeDtypeStruct((blocks, 3 * GROUP, LANES), jnp.float32),
        in_specs=[pl.BlockSpec(memory_space=pltpu.SMEM)] + [vmem] * 8,
        out_specs=vmem,
        scratch_shapes=[pltpu.VMEM(x.shape, x.dtype) for x in inner] + frame(members, columns),
        compiler_params=room(20),
        name="outer",
    )(places, *pieces, *inner, coriolis)


def gram_kernel(own, gathered_ref, value_ref, error_ref, out_ref, picks_ref, stack_ref):
    devices = gathered_ref.shape[0]
    members = 12
    spare = members // 3
    for d in range(devices):
        for f in range(3):
            at = d * members + f * spare
            picks_ref[at : at + spare, :] = gathered_ref[
                d, f * GROUP + members : (f + 1) * GROUP, :
            ]
    picks = picks_ref[...]
    hmean = jnp.mean(picks, axis=0, keepdims=True)
    scaled = (picks - hmean) / error_ref[...]
    misfit = (value_ref[...] - hmean) / error_ref[...]
    scaled_halves = halves(scaled)
    gram = product(scaled_halves, scaled_halves, ((1,), (1,)))
    drive = product(
        halves(jnp.broadcast_to(misfit, (8, LANES))), scaled_halves, ((1,), (1,))
    )
    n = LANES
    row = lax.broadcasted_iota(jnp.int32, (n, n), 0)
    column = lax.broadcasted_iota(jnp.int32, (n, n), 1)
    middle = gram[n : 2 * n, n : 2 * n]
    diagonal = jnp.sum(jnp.where(row == column, middle, 0.0), axis=0, keepdims=True)
    last = gram[2 * n :, 2 * n :]
    vectors = [jnp.broadcast_to(diagonal, (8, n))]
    vectors += [drive[:, k * n : (k + 1) * n] for k in range(3)]
    for k, vector in enumerate(vectors):
        turned = pltpu.roll(vector, n // 2, 1)
        left = column < n // 2
        last = jnp.where((row == n - 8 + 2 * k) & left, vector[0:1], last)
        last = jnp.where((row == n - 7 + 2 * k) & left, turned[0:1], last)
    blocks = (
        gram[0:n, n : 2 * n],
        gram[0:n, 2 * n :],
        gram[n : 2 * n, 2 * n :],
        jnp.where(row <= column, gram[0:n, 0:n], middle),
        last,
    )
    quads = n // 4
    for k, block in enumerate(blocks):
        stack_ref[k * quads : (k + 1) * quads] = block.reshape(quads, 4, n)
    size = out_ref.shape[1]
    piece = stack_ref[pl.ds(own[0] * size, size)]
    out_ref[...] = jnp.broadcast_to(piece[None], out_ref.shape)


def gram_piece(own, gathered, value, error, slabs):
    devices = gathered.shape[0]
    ens = 3 * LANES
    size = 5 * LANES // 4 // devices
    vmem = pl.BlockSpec(memory_space=pltpu.VMEM)
    return pl.pallas_call(
        gram_kernel,
        out_shape=jax.ShapeDtypeStruct((slabs, size, 4, LANES), jnp.float32),
        in_specs=[pl.BlockSpec(memory_space=pltpu.SMEM), vmem, vmem, vmem],
        out_specs=vmem,
        scratch_shapes=[
            pltpu.VMEM((ens, LANES), jnp.float32),
            pltpu.VMEM((5 * LANES // 4, 4, LANES), jnp.float32),
        ],
        compiler_params=room(8),
        name="gram",
    )(own, gathered, value, error)


def total_kernel(parts_ref, out_ref):
    total = jnp.sum(parts_ref[...], axis=0, keepdims=True)
    out_ref[...] = jnp.broadcast_to(total, out_ref.shape)


def total_piece(parts, devices):
    vmem = pl.BlockSpec(memory_space=pltpu.VMEM)
    return pl.pallas_call(
        total_kernel,
        out_shape=jax.ShapeDtypeStruct((devices, *parts.shape[1:]), jnp.float32),
        in_specs=[vmem],
        out_specs=vmem,
        compiler_params=room(8),
        name="total",
    )(parts)


def analysis_kernel(stack_ref, gathered_ref, out_ref, gram_ref, field_ref):
    n = LANES
    ens = 3 * n
    devices = gathered_ref.shape[0]
    members = ens // devices
    quads = members // 4
    row = lax.broadcasted_iota(jnp.int32, (n, n), 0)
    column = lax.broadcasted_iota(jnp.int32, (n, n), 1)

    def block(k):
        return stack_ref[k * n // 4 : (k + 1) * n // 4].reshape(n, n)

    for k, (i, j) in enumerate(((0, 1), (0, 2), (1, 2))):
        gram_ref[i * n : (i + 1) * n, j * n : (j + 1) * n] = block(k)
        gram_ref[j * n : (j + 1) * n, i * n : (i + 1) * n] = block(k).T
    both = block(3)
    upper = jnp.where(row < column, both, 0.0)
    gram_ref[0:n, 0:n] = upper + upper.T + jnp.where(row == column, both, 0.0)
    lower = jnp.where(row > column, both, 0.0)
    last = block(4)
    tail = last[n - 8 :]
    turned = pltpu.roll(tail, n // 2, 1)
    left = column[0:1] < n // 2
    vectors = [
        jnp.where(left, tail[2 * k : 2 * k + 1], turned[2 * k + 1 : 2 * k + 2]) for k in range(4)
    ]
    middle = jnp.where(row == column, vectors[0], 0.0)
    gram_ref[n : 2 * n, n : 2 * n] = lower + lower.T + middle
    upper = jnp.where(row < column, last, 0.0)
    gram_ref[2 * n :, 2 * n :] = upper + upper.T + jnp.where(row == column, last, 0.0)
    drive = jnp.concatenate(vectors[1:], axis=1)

    same = lax.broadcasted_iota(jnp.int32, (ens, ens), 0) == lax.broadcasted_iota(
        jnp.int32, (ens, ens), 1
    )
    identity = jnp.where(same, 1.0, 0.0)
    system = identity + gram_ref[...] * (1.0 / (ens - 1))
    norm_scale = jnp.sqrt(jnp.sum(system * system, keepdims=True))
    whole = system / norm_scale
    inverse = None
    for pair in range(NS_ITERS // 2):
        whole_halves = halves(whole)
        square = product(whole_halves, whole_halves)
        inner = 1.6875 * identity - 0.5625 * whole + 0.0625 * square
        quartic = product(halves(inner), halves(square)) + (2.25 * identity - 2.4375 * whole)
        quartic_halves = halves(quartic)
        inverse = quartic if pair == 0 else product(halves(inverse), quartic_halves)
        if 2 * pair + 2 < NS_ITERS:
            growth = product(quartic_halves, quartic_halves)
            whole = product(whole_halves, halves(growth))
    weights = inverse / jnp.sqrt(norm_scale)
    pulled = jnp.sum(weights * drive, axis=1, keepdims=True)
    mean_weight = jnp.sum(weights * pulled, axis=0, keepdims=True) * (1.0 / (ens - 1))
    combined = halves(weights + mean_weight)

    for f in range(3):
        for d in range(devices):
            field_ref[f, d * members : (d + 1) * members, :] = gathered_ref[
                d, f * GROUP : f * GROUP + members, :
            ]
    for f in range(3):
        field = field_ref[f]
        center = jnp.mean(field, axis=0, keepdims=True)
        field_ref[f] = center + product(combined, halves(field - center))
    for f in range(3):
        for d in range(devices):
            part = field_ref[f, d * members : (d + 1) * members, :]
            out_ref[d, f * quads : (f + 1) * quads] = part.reshape(quads, 4, n)


def analysis(stack, gathered):
    devices = gathered.shape[0]
    ens = 3 * LANES
    vmem = pl.BlockSpec(memory_space=pltpu.VMEM)
    return pl.pallas_call(
        analysis_kernel,
        out_shape=jax.ShapeDtypeStruct((devices, 3 * ens // devices // 4, 4, LANES), jnp.float32),
        in_specs=[vmem, vmem],
        out_specs=vmem,
        scratch_shapes=[
            pltpu.VMEM((ens, ens), jnp.float32),
            pltpu.VMEM((3, ens, LANES), jnp.float32),
        ],
        compiler_params=room(16),
        name="analysis",
    )(stack, gathered)


def local(ensemble, sea_depth, ocean_mask, observed_cells, observed_values, observed_error):
    local_members, fields, rows_here, columns = ensemble.shape
    devices = lax.axis_size(MEM)
    slabs = lax.axis_size("space")
    coriolis = 0.05 + 0.1 * jnp.arange(columns, dtype=jnp.float32)[None] / columns
    cells = observed_cells[0]
    places = jnp.stack(
        [
            cells // columns,
            cells % columns // LANES * LANES,
            (jnp.arange(LANES, dtype=jnp.int32) - cells) % LANES,
        ]
    )
    own = lax.axis_index(MEM).astype(jnp.int32).reshape(1)
    planes = planes_of(ensemble, sea_depth, ocean_mask)
    edge = HALO - rows_here
    before = lax.ppermute(planes, "space", ring("space", 1))
    after = lax.ppermute(planes, "space", ring("space", -1))
    far_before = lax.ppermute(planes[rows_here - edge :], "space", ring("space", 2))
    far_after = lax.ppermute(planes[:edge], "space", ring("space", -2))
    inner = inner_rows((before, planes, after), coriolis, local_members)
    pieces = (far_before, before, planes, after, far_after)
    sent = forecast(places, pieces, inner, coriolis, local_members, devices)
    gathered = lax.all_to_all(sent, MEM, 0, 0, tiled=True)
    parts = gram_piece(own, gathered, observed_values, observed_error, slabs)
    parts = lax.all_to_all(parts, "space", 0, 0, tiled=True)
    pieces = lax.all_to_all(total_piece(parts, devices), MEM, 0, 0, tiled=True)
    result = analysis(pieces.reshape(-1, 4, LANES), gathered)
    returned = lax.all_to_all(result, MEM, 0, 0, tiled=True)
    returned = returned.reshape(rows_here, columns // LANES, fields, local_members, LANES)
    return returned.transpose(3, 2, 0, 1, 4).reshape(ensemble.shape)


def solution(mesh):
    finer = Mesh(mesh.devices.reshape(8, 4, mesh.shape["space"]), ("mem_0", "mem_1", "space"))
    return jax.shard_map(
        local,
        mesh=finer,
        in_specs=(
            P(MEM, None, "space", None),
            P("space", None),
            P("space", None),
            P("space", None),
            P("space", None),
            P("space", None),
        ),
        out_specs=P(MEM, None, "space", None),
        check_vma=False,
    )
```

```python
import functools

import jax
import jax.numpy as jnp
from jax import lax
from jax.experimental import pallas as pl
from jax.experimental.pallas import tpu as pltpu
from jax.sharding import Mesh
from jax.sharding import PartitionSpec as P

STEPS = 3
NS_ITERS = 6
MEM = ("mem_0", "mem_1")

GRAV = 1.0
DT = 0.3
VISC = 0.1

LANES = 128
GROUP = 16
HALO = 2 * STEPS


def ring(axis, turn):
    count = lax.axis_size(axis)
    return [(i, (i + turn) % count) for i in range(count)]


def halves(x):
    top = x.astype(jnp.bfloat16)
    return top, (x - top.astype(jnp.float32)).astype(jnp.bfloat16)


def product(a, b, contract=((1,), (0,))):
    left = jnp.concatenate([a[0], a[0], a[1]], axis=contract[0][0])
    right = jnp.concatenate([b[0], b[1], b[0]], axis=contract[1][0])
    return lax.dot_general(left, right, (contract, ((), ())), preferred_element_type=jnp.float32)


def room(mebibytes):
    return pltpu.CompilerParams(vmem_limit_bytes=mebibytes << 20)


def planes_kernel(state_hbm, depth_hbm, ocean_hbm, out_ref, state_ref, depth_ref, ocean_ref, sems):
    members, fields, rows, columns = state_ref.shape
    copies = [
        pltpu.make_async_copy(source, target, sems.at[k])
        for k, (source, target) in enumerate(
            ((depth_hbm, depth_ref), (ocean_hbm, ocean_ref), (state_hbm, state_ref))
        )
    ]
    for copy in copies:
        copy.start()
    copies[0].wait()
    copies[1].wait()
    at = fields * members
    depth = depth_ref[...]
    ocean = ocean_ref[...].astype(jnp.float32)
    for r in range(rows):
        out_ref[r, at : at + 1, :] = depth[r : r + 1]
        out_ref[r, at + 1 : at + 2, :] = ocean[r : r + 1]
        out_ref[r, at + 2 : at + 4, :] = jnp.zeros((2, columns), jnp.float32)
    copies[2].wait()
    for f in range(fields):
        for m in range(members):
            at = f * members + m
            plane = state_ref[m, f]
            for r in range(rows):
                out_ref[r, at : at + 1, :] = plane[r : r + 1]


def planes_of(state, depth, ocean):
    members, fields, rows, columns = state.shape
    return pl.pallas_call(
        planes_kernel,
        out_shape=jax.ShapeDtypeStruct((rows, fields * members + 4, columns), jnp.float32),
        in_specs=[pl.BlockSpec(memory_space=pltpu.HBM)] * 3,
        out_specs=pl.BlockSpec(memory_space=pltpu.VMEM),
        scratch_shapes=[
            pltpu.VMEM(state.shape, jnp.float32),
            pltpu.VMEM(depth.shape, jnp.float32),
            pltpu.VMEM(ocean.shape, jnp.int32),
            pltpu.SemaphoreType.DMA((3,)),
        ],
        compiler_params=room(8),
        name="planes",
    )(*(pltpu.with_memory_space_constraint(x, pltpu.HBM) for x in (state, depth, ocean)))


def north(x):
    return pltpu.roll(x, x.shape[1] - 1, 1)


def south(x):
    return pltpu.roll(x, 1, 1)


def sublane_parts(members):
    return [slice(at, min(at + 8, members)) for at in range(0, members, 8)]


def rows_of(ref, inner=None, first=0, last=-1):
    def get(f, r, m):
        return (inner if inner is not None and first <= r <= last else ref)[f, r, m]

    return get


def advance(get, target, still, fresh_ref, coriolis, first, last, known=None):
    parts = sublane_parts(target.shape[2])

    def height_row(r):
        depth_above = still[r + 1, 0:1]
        depth_below = still[r - 1, 0:1]
        depth = still[r, 0:1]
        for m in parts:
            above = (depth_above + get(0, r + 1, m)) * get(1, r + 1, m)
            below = (depth_below + get(0, r - 1, m)) * get(1, r - 1, m)
            height = get(0, r, m)
            across = (depth + height) * get(2, r, m)
            fresh_ref[r, m] = height - (0.5 * DT) * (
                (above - below) + (north(across) - south(across))
            )

    low = first if known == first - 1 else first - 1
    high = last if known == last + 1 else last + 1
    for r in range(low, high + 1):
        height_row(r)

    def flow_row(r):
        ocean = still[r, 1:2]
        for m in parts:
            u, v = get(1, r, m), get(2, r, m)
            ue, uw = get(1, r + 1, m), get(1, r - 1, m)
            un, us = north(u), south(u)
            tend = GRAV * (fresh_ref[r + 1, m] - fresh_ref[r - 1, m])
            tend = tend + u * (ue - uw) + v * (un - us)
            new = (1.0 - 4.0 * DT * VISC) * u - (0.5 * DT) * tend + coriolis * v
            target[1, r, m] = (new + (DT * VISC) * ((ue + uw) + (un + us))) * ocean
            fresh = fresh_ref[r, m]
            target[0, r, m] = fresh
            ve, vw = get(2, r + 1, m), get(2, r - 1, m)
            vn, vs = north(v), south(v)
            tend = GRAV * (north(fresh) - south(fresh)) + u * (ve - vw) + v * (vn - vs)
            new = (1.0 - 4.0 * DT * VISC) * v - (0.5 * DT) * tend - coriolis * u
            target[2, r, m] = (new + (DT * VISC) * ((ve + vw) + (vn + vs))) * ocean

    for r in range(first, last + 1):
        flow_row(r)


def unpack(piece, count, at, state_ref, still_ref):
    members = state_ref.shape[2]
    for r in range(count):
        for f in range(3):
            state_ref[f, at + r] = piece[r, f * members : (f + 1) * members, :]
        still_ref[at + r] = piece[r, 3 * members : 3 * members + 2, :]


def inner_kernel(
    before_ref, own_ref, after_ref, coriolis_ref, a_ref, b_ref, raw_ref, fresh_ref, still_ref
):
    coriolis = coriolis_ref[...] * DT
    for at, piece in ((2, before_ref), (6, own_ref), (10, after_ref)):
        unpack(piece, 4, at, raw_ref, still_ref)
    advance(rows_of(raw_ref), a_ref, still_ref, fresh_ref, coriolis, 4, 11)
    advance(rows_of(a_ref), b_ref, still_ref, fresh_ref, coriolis, 6, 9)


def outer_kernel(
    places,
    far_before_ref,
    before_ref,
    own_ref,
    after_ref,
    far_after_ref,
    one_ref,
    two_ref,
    coriolis_ref,
    out_ref,
    a_ref,
    b_ref,
    raw_ref,
    fresh_ref,
    still_ref,
):
    members, columns = raw_ref.shape[2:]
    rows_here = own_ref.shape[0]
    coriolis = coriolis_ref[...] * DT
    for at, piece in ((0, far_before_ref), (2, before_ref), (10, after_ref), (14, far_after_ref)):
        unpack(piece, piece.shape[0], at, raw_ref, still_ref)
    for r in range(rows_here):
        still_ref[6 + r] = own_ref[r, 3 * members : 3 * members + 2, :]
    raw = rows_of(raw_ref)
    one = rows_of(a_ref, one_ref, 4, 11)
    two = rows_of(b_ref, two_ref, 6, 9)
    for r in (4, 11):
        fresh_ref[r] = one_ref[0, r]
    advance(raw, a_ref, still_ref, fresh_ref, coriolis, 2, 3, 4)
    advance(raw, a_ref, still_ref, fresh_ref, coriolis, 12, 13, 11)
    for r in (6, 9):
        fresh_ref[r] = two_ref[0, r]
    advance(one, b_ref, still_ref, fresh_ref, coriolis, 4, 5, 6)
    advance(one, b_ref, still_ref, fresh_ref, coriolis, 10, 11, 9)
    advance(two, raw_ref, still_ref, fresh_ref, coriolis, 6, 9)
    source = raw_ref
    lane = lax.broadcasted_iota(jnp.int32, (members, LANES), 1)

    def pick(o, found):
        start = pl.multiple_of(places[1, o], LANES)
        block = source[0, HALO + places[0, o], :, pl.ds(start, LANES)]
        return jnp.where(lane == o, pltpu.roll(block, places[2, o], 1), found)

    picks = lax.fori_loop(0, LANES, pick, jnp.zeros((members, LANES), jnp.float32), unroll=8)
    per_row = columns // LANES
    spare = members // 3
    for f in range(3):
        part = picks[f * spare : (f + 1) * spare]
        for r in range(rows_here):
            for c in range(per_row):
                d = r * per_row + c
                out_ref[d, f * GROUP : f * GROUP + members, :] = source[
                    f, HALO + r, :, c * LANES : (c + 1) * LANES
                ]
                out_ref[d, f * GROUP + members : (f + 1) * GROUP, :] = part


def frame(members, columns):
    rows = 2 * HALO + 4
    return [
        pltpu.VMEM((3, rows, members, columns), jnp.float32),
        pltpu.VMEM((rows, members, columns), jnp.float32),
        pltpu.VMEM((rows, 2, columns), jnp.float32),
    ]


def inner_rows(near, coriolis, members):
    columns = near[0].shape[2]
    vmem = pl.BlockSpec(memory_space=pltpu.VMEM)
    return pl.pallas_call(
        inner_kernel,
        out_shape=(
            jax.ShapeDtypeStruct((3, 2 * HALO + 4, members, columns), jnp.float32),
        ) * 2,
        in_specs=[vmem] * 4,
        out_specs=(vmem, vmem),
        scratch_shapes=frame(members, columns),
        compiler_params=room(20),
        name="inner",
    )(*near, coriolis)


def forecast(places, pieces, inner, coriolis, members, blocks):
    columns = pieces[0].shape[2]
    vmem = pl.BlockSpec(memory_space=pltpu.VMEM)
    return pl.pallas_call(
        outer_kernel,
        out_shape=jax.ShapeDtypeStruct((blocks, 3 * GROUP, LANES), jnp.float32),
        in_specs=[pl.BlockSpec(memory_space=pltpu.SMEM)] + [vmem] * 8,
        out_specs=vmem,
        scratch_shapes=[pltpu.VMEM(x.shape, x.dtype) for x in inner] + frame(members, columns),
        compiler_params=room(20),
        name="outer",
    )(places, *pieces, *inner, coriolis)


def gram_kernel(own, gathered_ref, value_ref, error_ref, out_ref, picks_ref, stack_ref):
    devices = gathered_ref.shape[0]
    members = 12
    spare = members // 3
    for d in range(devices):
        for f in range(3):
            at = d * members + f * spare
            picks_ref[at : at + spare, :] = gathered_ref[
                d, f * GROUP + members : (f + 1) * GROUP, :
            ]
    picks = picks_ref[...]
    hmean = jnp.mean(picks, axis=0, keepdims=True)
    scaled = (picks - hmean) / error_ref[...]
    misfit = (value_ref[...] - hmean) / error_ref[...]
    scaled_halves = halves(scaled)
    gram = product(scaled_halves, scaled_halves, ((1,), (1,)))
    drive = product(
        halves(jnp.broadcast_to(misfit, (8, LANES))), scaled_halves, ((1,), (1,))
    )
    n = LANES
    row = lax.broadcasted_iota(jnp.int32, (n, n), 0)
    column = lax.broadcasted_iota(jnp.int32, (n, n), 1)
    middle = gram[n : 2 * n, n : 2 * n]
    diagonal = jnp.sum(jnp.where(row == column, middle, 0.0), axis=0, keepdims=True)
    last = gram[2 * n :, 2 * n :]
    vectors = [jnp.broadcast_to(diagonal, (8, n))]
    vectors += [drive[:, k * n : (k + 1) * n] for k in range(3)]
    for k, vector in enumerate(vectors):
        turned = pltpu.roll(vector, n // 2, 1)
        left = column < n // 2
        last = jnp.where((row == n - 8 + 2 * k) & left, vector[0:1], last)
        last = jnp.where((row == n - 7 + 2 * k) & left, turned[0:1], last)
    blocks = (
        gram[0:n, n : 2 * n],
        gram[0:n, 2 * n :],
        gram[n : 2 * n, 2 * n :],
        jnp.where(row <= column, gram[0:n, 0:n], middle),
        last,
    )
    quads = n // 4
    for k, block in enumerate(blocks):
        stack_ref[k * quads : (k + 1) * quads] = block.reshape(quads, 4, n)
    size = out_ref.shape[1]
    piece = stack_ref[pl.ds(own[0] * size, size)]
    out_ref[...] = jnp.broadcast_to(piece[None], out_ref.shape)


def gram_piece(own, gathered, value, error, slabs):
    devices = gathered.shape[0]
    ens = 3 * LANES
    size = 5 * LANES // 4 // devices
    vmem = pl.BlockSpec(memory_space=pltpu.VMEM)
    return pl.pallas_call(
        gram_kernel,
        out_shape=jax.ShapeDtypeStruct((slabs, size, 4, LANES), jnp.float32),
        in_specs=[pl.BlockSpec(memory_space=pltpu.SMEM), vmem, vmem, vmem],
        out_specs=vmem,
        scratch_shapes=[
            pltpu.VMEM((ens, LANES), jnp.float32),
            pltpu.VMEM((5 * LANES // 4, 4, LANES), jnp.float32),
        ],
        compiler_params=room(8),
        name="gram",
    )(own, gathered, value, error)


def total_kernel(parts_ref, out_ref):
    total = jnp.sum(parts_ref[...], axis=0, keepdims=True)
    out_ref[...] = jnp.broadcast_to(total, out_ref.shape)


def total_piece(parts, devices):
    vmem = pl.BlockSpec(memory_space=pltpu.VMEM)
    return pl.pallas_call(
        total_kernel,
        out_shape=jax.ShapeDtypeStruct((devices, *parts.shape[1:]), jnp.float32),
        in_specs=[vmem],
        out_specs=vmem,
        compiler_params=room(8),
        name="total",
    )(parts)


def analysis_kernel(stack_ref, gathered_ref, out_ref, gram_ref, field_ref):
    n = LANES
    ens = 3 * n
    devices = gathered_ref.shape[0]
    members = ens // devices
    quads = members // 4
    row = lax.broadcasted_iota(jnp.int32, (n, n), 0)
    column = lax.broadcasted_iota(jnp.int32, (n, n), 1)

    def block(k):
        return stack_ref[k * n // 4 : (k + 1) * n // 4].reshape(n, n)

    for k, (i, j) in enumerate(((0, 1), (0, 2), (1, 2))):
        gram_ref[i * n : (i + 1) * n, j * n : (j + 1) * n] = block(k)
        gram_ref[j * n : (j + 1) * n, i * n : (i + 1) * n] = block(k).T
    both = block(3)
    upper = jnp.where(row < column, both, 0.0)
    gram_ref[0:n, 0:n] = upper + upper.T + jnp.where(row == column, both, 0.0)
    lower = jnp.where(row > column, both, 0.0)
    last = block(4)
    tail = last[n - 8 :]
    turned = pltpu.roll(tail, n // 2, 1)
    left = column[0:1] < n // 2
    vectors = [
        jnp.where(left, tail[2 * k : 2 * k + 1], turned[2 * k + 1 : 2 * k + 2]) for k in range(4)
    ]
    middle = jnp.where(row == column, vectors[0], 0.0)
    gram_ref[n : 2 * n, n : 2 * n] = lower + lower.T + middle
    upper = jnp.where(row < column, last, 0.0)
    gram_ref[2 * n :, 2 * n :] = upper + upper.T + jnp.where(row == column, last, 0.0)
    drive = jnp.concatenate(vectors[1:], axis=1)

    same = lax.broadcasted_iota(jnp.int32, (ens, ens), 0) == lax.broadcasted_iota(
        jnp.int32, (ens, ens), 1
    )
    identity = jnp.where(same, 1.0, 0.0)
    system = identity + gram_ref[...] * (1.0 / (ens - 1))
    norm_scale = jnp.sqrt(jnp.sum(system * system, keepdims=True))
    whole = system / norm_scale
    inverse = None
    for pair in range(NS_ITERS // 2):
        whole_halves = halves(whole)
        square = product(whole_halves, whole_halves)
        inner = 1.6875 * identity - 0.5625 * whole + 0.0625 * square
        quartic = product(halves(inner), halves(square)) + (2.25 * identity - 2.4375 * whole)
        quartic_halves = halves(quartic)
        inverse = quartic if pair == 0 else product(halves(inverse), quartic_halves)
        if 2 * pair + 2 < NS_ITERS:
            growth = product(quartic_halves, quartic_halves)
            whole = product(whole_halves, halves(growth))
    weights = inverse / jnp.sqrt(norm_scale)
    pulled = jnp.sum(weights * drive, axis=1, keepdims=True)
    mean_weight = jnp.sum(weights * pulled, axis=0, keepdims=True) * (1.0 / (ens - 1))
    combined = halves(weights + mean_weight)

    for f in range(3):
        for d in range(devices):
            field_ref[f, d * members : (d + 1) * members, :] = gathered_ref[
                d, f * GROUP : f * GROUP + members, :
            ]
    for f in range(3):
        field = field_ref[f]
        center = jnp.mean(field, axis=0, keepdims=True)
        field_ref[f] = center + product(combined, halves(field - center))
    for f in range(3):
        for d in range(devices):
            part = field_ref[f, d * members : (d + 1) * members, :]
            out_ref[d, f * quads : (f + 1) * quads] = part.reshape(quads, 4, n)


def analysis(stack, gathered):
    devices = gathered.shape[0]
    ens = 3 * LANES
    vmem = pl.BlockSpec(memory_space=pltpu.VMEM)
    return pl.pallas_call(
        analysis_kernel,
        out_shape=jax.ShapeDtypeStruct((devices, 3 * ens // devices // 4, 4, LANES), jnp.float32),
        in_specs=[vmem, vmem],
        out_specs=vmem,
        scratch_shapes=[
            pltpu.VMEM((ens, ens), jnp.float32),
            pltpu.VMEM((3, ens, LANES), jnp.float32),
        ],
        compiler_params=room(16),
        name="analysis",
    )(stack, gathered)


def local(ensemble, sea_depth, ocean_mask, observed_cells, observed_values, observed_error):
    local_members, fields, rows_here, columns = ensemble.shape
    devices = lax.axis_size(MEM)
    slabs = lax.axis_size("space")
    coriolis = 0.05 + 0.1 * jnp.arange(columns, dtype=jnp.float32)[None] / columns
    cells = observed_cells[0]
    places = jnp.stack(
        [
            cells // columns,
            cells % columns // LANES * LANES,
            (jnp.arange(LANES, dtype=jnp.int32) - cells) % LANES,
        ]
    )
    own = lax.axis_index(MEM).astype(jnp.int32).reshape(1)
    planes = planes_of(ensemble, sea_depth, ocean_mask)
    edge = HALO - rows_here
    before = lax.ppermute(planes, "space", ring("space", 1))
    after = lax.ppermute(planes, "space", ring("space", -1))
    far_before = lax.ppermute(planes[rows_here - edge :], "space", ring("space", 2))
    far_after = lax.ppermute(planes[:edge], "space", ring("space", -2))
    inner = inner_rows((before, planes, after), coriolis, local_members)
    pieces = (far_before, before, planes, after, far_after)
    sent = forecast(places, pieces, inner, coriolis, local_members, devices)
    gathered = lax.all_to_all(sent, MEM, 0, 0, tiled=True)
    parts = gram_piece(own, gathered, observed_values, observed_error, slabs)
    parts = lax.all_to_all(parts, "space", 0, 0, tiled=True)
    pieces = lax.all_to_all(total_piece(parts, devices), MEM, 0, 0, tiled=True)
    result = analysis(pieces.reshape(-1, 4, LANES), gathered)
    returned = lax.all_to_all(result, MEM, 0, 0, tiled=True)
    returned = returned.reshape(rows_here, columns // LANES, fields, local_members, LANES)
    return returned.transpose(3, 2, 0, 1, 4).reshape(ensemble.shape)


def solution(mesh):
    finer = Mesh(mesh.devices.reshape(8, 4, mesh.shape["space"]), ("mem_0", "mem_1", "space"))
    return jax.shard_map(
        local,
        mesh=finer,
        in_specs=(
            P(MEM, None, "space", None),
            P("space", None),
            P("space", None),
            P("space", None),
            P("space", None),
            P("space", None),
        ),
        out_specs=P(MEM, None, "space", None),
        check_vma=False,
    )
```

```python
import functools

import jax
import jax.numpy as jnp
from jax import lax
from jax.experimental import pallas as pl
from jax.experimental.pallas import tpu as pltpu
from jax.sharding import Mesh
from jax.sharding import PartitionSpec as P

STEPS = 3
NS_ITERS = 6
MEM = ("mem_0", "mem_1")

GRAV = 1.0
DT = 0.3
VISC = 0.1

LANES = 128
GROUP = 16
HALO = 2 * STEPS


def ring(axis, turn):
    count = lax.axis_size(axis)
    return [(i, (i + turn) % count) for i in range(count)]


def halves(x):
    top = x.astype(jnp.bfloat16)
    return top, (x - top.astype(jnp.float32)).astype(jnp.bfloat16)


def product(a, b, contract=((1,), (0,))):
    left = jnp.concatenate([a[0], a[0], a[1]], axis=contract[0][0])
    right = jnp.concatenate([b[0], b[1], b[0]], axis=contract[1][0])
    return lax.dot_general(left, right, (contract, ((), ())), preferred_element_type=jnp.float32)


def room(mebibytes):
    return pltpu.CompilerParams(vmem_limit_bytes=mebibytes << 20)


def planes_kernel(state_hbm, depth_hbm, ocean_hbm, out_ref, state_ref, depth_ref, ocean_ref, sems):
    members, fields, rows, columns = state_ref.shape
    copies = [
        pltpu.make_async_copy(source, target, sems.at[k])
        for k, (source, target) in enumerate(
            ((depth_hbm, depth_ref), (ocean_hbm, ocean_ref), (state_hbm, state_ref))
        )
    ]
    for copy in copies:
        copy.start()
    copies[0].wait()
    copies[1].wait()
    at = fields * members
    depth = depth_ref[...]
    ocean = ocean_ref[...].astype(jnp.float32)
    for r in range(rows):
        out_ref[r, at : at + 1, :] = depth[r : r + 1]
        out_ref[r, at + 1 : at + 2, :] = ocean[r : r + 1]
        out_ref[r, at + 2 : at + 4, :] = jnp.zeros((2, columns), jnp.float32)
    copies[2].wait()
    for f in range(fields):
        for m in range(members):
            at = f * members + m
            plane = state_ref[m, f]
            for r in range(rows):
                out_ref[r, at : at + 1, :] = plane[r : r + 1]


def planes_of(state, depth, ocean):
    members, fields, rows, columns = state.shape
    return pl.pallas_call(
        planes_kernel,
        out_shape=jax.ShapeDtypeStruct((rows, fields * members + 4, columns), jnp.float32),
        in_specs=[pl.BlockSpec(memory_space=pltpu.HBM)] * 3,
        out_specs=pl.BlockSpec(memory_space=pltpu.VMEM),
        scratch_shapes=[
            pltpu.VMEM(state.shape, jnp.float32),
            pltpu.VMEM(depth.shape, jnp.float32),
            pltpu.VMEM(ocean.shape, jnp.int32),
            pltpu.SemaphoreType.DMA((3,)),
        ],
        compiler_params=room(8),
        name="planes",
    )(*(pltpu.with_memory_space_constraint(x, pltpu.HBM) for x in (state, depth, ocean)))


def north(x):
    return pltpu.roll(x, x.shape[1] - 1, 1)


def south(x):
    return pltpu.roll(x, 1, 1)


def sublane_parts(members):
    return [slice(at, min(at + 8, members)) for at in range(0, members, 8)]


def rows_of(ref, inner=None, first=0, last=-1):
    def get(f, r, m):
        return (inner if inner is not None and first <= r <= last else ref)[f, r, m]

    return get


def advance(get, target, still, fresh_ref, coriolis, first, last, known=None):
    parts = sublane_parts(target.shape[2])

    def height_row(r):
        depth_above = still[r + 1, 0:1]
        depth_below = still[r - 1, 0:1]
        depth = still[r, 0:1]
        for m in parts:
            above = (depth_above + get(0, r + 1, m)) * get(1, r + 1, m)
            below = (depth_below + get(0, r - 1, m)) * get(1, r - 1, m)
            height = get(0, r, m)
            across = (depth + height) * get(2, r, m)
            fresh_ref[r, m] = height - (0.5 * DT) * (
                (above - below) + (north(across) - south(across))
            )

    low = first if known == first - 1 else first - 1
    high = last if known == last + 1 else last + 1
    for r in range(low, high + 1):
        height_row(r)

    def flow_row(r):
        ocean = still[r, 1:2]
        for m in parts:
            u, v = get(1, r, m), get(2, r, m)
            ue, uw = get(1, r + 1, m), get(1, r - 1, m)
            un, us = north(u), south(u)
            tend = GRAV * (fresh_ref[r + 1, m] - fresh_ref[r - 1, m])
            tend = tend + u * (ue - uw) + v * (un - us)
            new = (1.0 - 4.0 * DT * VISC) * u - (0.5 * DT) * tend + coriolis * v
            target[1, r, m] = (new + (DT * VISC) * ((ue + uw) + (un + us))) * ocean
            fresh = fresh_ref[r, m]
            target[0, r, m] = fresh
            ve, vw = get(2, r + 1, m), get(2, r - 1, m)
            vn, vs = north(v), south(v)
            tend = GRAV * (north(fresh) - south(fresh)) + u * (ve - vw) + v * (vn - vs)
            new = (1.0 - 4.0 * DT * VISC) * v - (0.5 * DT) * tend - coriolis * u
            target[2, r, m] = (new + (DT * VISC) * ((ve + vw) + (vn + vs))) * ocean

    for r in range(first, last + 1):
        flow_row(r)


def unpack(piece, count, at, state_ref, still_ref):
    members = state_ref.shape[2]
    for r in range(count):
        for f in range(3):
            state_ref[f, at + r] = piece[r, f * members : (f + 1) * members, :]
        still_ref[at + r] = piece[r, 3 * members : 3 * members + 2, :]


def inner_kernel(
    before_ref, own_ref, after_ref, coriolis_ref, a_ref, b_ref, raw_ref, fresh_ref, still_ref
):
    coriolis = coriolis_ref[...] * DT
    for at, piece in ((2, before_ref), (6, own_ref), (10, after_ref)):
        unpack(piece, 4, at, raw_ref, still_ref)
    advance(rows_of(raw_ref), a_ref, still_ref, fresh_ref, coriolis, 4, 11)
    advance(rows_of(a_ref), b_ref, still_ref, fresh_ref, coriolis, 6, 9)


def outer_kernel(
    places,
    far_before_ref,
    before_ref,
    own_ref,
    after_ref,
    far_after_ref,
    one_ref,
    two_ref,
    coriolis_ref,
    out_ref,
    a_ref,
    b_ref,
    raw_ref,
    fresh_ref,
    still_ref,
):
    members, columns = raw_ref.shape[2:]
    rows_here = own_ref.shape[0]
    coriolis = coriolis_ref[...] * DT
    for at, piece in ((0, far_before_ref), (2, before_ref), (10, after_ref), (14, far_after_ref)):
        unpack(piece, piece.shape[0], at, raw_ref, still_ref)
    for r in range(rows_here):
        still_ref[6 + r] = own_ref[r, 3 * members : 3 * members + 2, :]
    raw = rows_of(raw_ref)
    one = rows_of(a_ref, one_ref, 4, 11)
    two = rows_of(b_ref, two_ref, 6, 9)
    for r in (4, 11):
        fresh_ref[r] = one_ref[0, r]
    advance(raw, a_ref, still_ref, fresh_ref, coriolis, 2, 3, 4)
    advance(raw, a_ref, still_ref, fresh_ref, coriolis, 12, 13, 11)
    for r in (6, 9):
        fresh_ref[r] = two_ref[0, r]
    advance(one, b_ref, still_ref, fresh_ref, coriolis, 4, 5, 6)
    advance(one, b_ref, still_ref, fresh_ref, coriolis, 10, 11, 9)
    advance(two, raw_ref, still_ref, fresh_ref, coriolis, 6, 9)
    source = raw_ref
    lane = lax.broadcasted_iota(jnp.int32, (members, LANES), 1)

    def pick(o, found):
        start = pl.multiple_of(places[1, o], LANES)
        block = source[0, HALO + places[0, o], :, pl.ds(start, LANES)]
        return jnp.where(lane == o, pltpu.roll(block, places[2, o], 1), found)

    picks = lax.fori_loop(0, LANES, pick, jnp.zeros((members, LANES), jnp.float32), unroll=32)
    per_row = columns // LANES
    spare = members // 3
    for f in range(3):
        part = picks[f * spare : (f + 1) * spare]
        for r in range(rows_here):
            for c in range(per_row):
                d = r * per_row + c
                out_ref[d, f * GROUP : f * GROUP + members, :] = source[
                    f, HALO + r, :, c * LANES : (c + 1) * LANES
                ]
                out_ref[d, f * GROUP + members : (f + 1) * GROUP, :] = part


def frame(members, columns):
    rows = 2 * HALO + 4
    return [
        pltpu.VMEM((3, rows, members, columns), jnp.float32),
        pltpu.VMEM((rows, members, columns), jnp.float32),
        pltpu.VMEM((rows, 2, columns), jnp.float32),
    ]


def inner_rows(near, coriolis, members):
    columns = near[0].shape[2]
    vmem = pl.BlockSpec(memory_space=pltpu.VMEM)
    return pl.pallas_call(
        inner_kernel,
        out_shape=(
            jax.ShapeDtypeStruct((3, 2 * HALO + 4, members, columns), jnp.float32),
        ) * 2,
        in_specs=[vmem] * 4,
        out_specs=(vmem, vmem),
        scratch_shapes=frame(members, columns),
        compiler_params=room(20),
        name="inner",
    )(*near, coriolis)


def forecast(places, pieces, inner, coriolis, members, blocks):
    columns = pieces[0].shape[2]
    vmem = pl.BlockSpec(memory_space=pltpu.VMEM)
    return pl.pallas_call(
        outer_kernel,
        out_shape=jax.ShapeDtypeStruct((blocks, 3 * GROUP, LANES), jnp.float32),
        in_specs=[pl.BlockSpec(memory_space=pltpu.SMEM)] + [vmem] * 8,
        out_specs=vmem,
        scratch_shapes=[pltpu.VMEM(x.shape, x.dtype) for x in inner] + frame(members, columns),
        compiler_params=room(20),
        name="outer",
    )(places, *pieces, *inner, coriolis)


def gram_kernel(own, gathered_ref, value_ref, error_ref, out_ref, picks_ref, stack_ref):
    devices = gathered_ref.shape[0]
    members = 12
    spare = members // 3
    for d in range(devices):
        for f in range(3):
            at = d * members + f * spare
            picks_ref[at : at + spare, :] = gathered_ref[
                d, f * GROUP + members : (f + 1) * GROUP, :
            ]
    picks = picks_ref[...]
    hmean = jnp.mean(picks, axis=0, keepdims=True)
    scaled = (picks - hmean) / error_ref[...]
    misfit = (value_ref[...] - hmean) / error_ref[...]
    scaled_halves = halves(scaled)
    gram = product(scaled_halves, scaled_halves, ((1,), (1,)))
    drive = product(
        halves(jnp.broadcast_to(misfit, (8, LANES))), scaled_halves, ((1,), (1,))
    )
    n = LANES
    row = lax.broadcasted_iota(jnp.int32, (n, n), 0)
    column = lax.broadcasted_iota(jnp.int32, (n, n), 1)
    middle = gram[n : 2 * n, n : 2 * n]
    diagonal = jnp.sum(jnp.where(row == column, middle, 0.0), axis=0, keepdims=True)
    last = gram[2 * n :, 2 * n :]
    vectors = [jnp.broadcast_to(diagonal, (8, n))]
    vectors += [drive[:, k * n : (k + 1) * n] for k in range(3)]
    for k, vector in enumerate(vectors):
        turned = pltpu.roll(vector, n // 2, 1)
        left = column < n // 2
        last = jnp.where((row == n - 8 + 2 * k) & left, vector[0:1], last)
        last = jnp.where((row == n - 7 + 2 * k) & left, turned[0:1], last)
    blocks = (
        gram[0:n, n : 2 * n],
        gram[0:n, 2 * n :],
        gram[n : 2 * n, 2 * n :],
        jnp.where(row <= column, gram[0:n, 0:n], middle),
        last,
    )
    quads = n // 4
    for k, block in enumerate(blocks):
        stack_ref[k * quads : (k + 1) * quads] = block.reshape(quads, 4, n)
    size = out_ref.shape[1]
    piece = stack_ref[pl.ds(own[0] * size, size)]
    out_ref[...] = jnp.broadcast_to(piece[None], out_ref.shape)


def gram_piece(own, gathered, value, error, slabs):
    devices = gathered.shape[0]
    ens = 3 * LANES
    size = 5 * LANES // 4 // devices
    vmem = pl.BlockSpec(memory_space=pltpu.VMEM)
    return pl.pallas_call(
        gram_kernel,
        out_shape=jax.ShapeDtypeStruct((slabs, size, 4, LANES), jnp.float32),
        in_specs=[pl.BlockSpec(memory_space=pltpu.SMEM), vmem, vmem, vmem],
        out_specs=vmem,
        scratch_shapes=[
            pltpu.VMEM((ens, LANES), jnp.float32),
            pltpu.VMEM((5 * LANES // 4, 4, LANES), jnp.float32),
        ],
        compiler_params=room(8),
        name="gram",
    )(own, gathered, value, error)


def total_kernel(parts_ref, out_ref):
    total = jnp.sum(parts_ref[...], axis=0, keepdims=True)
    out_ref[...] = jnp.broadcast_to(total, out_ref.shape)


def total_piece(parts, devices):
    vmem = pl.BlockSpec(memory_space=pltpu.VMEM)
    return pl.pallas_call(
        total_kernel,
        out_shape=jax.ShapeDtypeStruct((devices, *parts.shape[1:]), jnp.float32),
        in_specs=[vmem],
        out_specs=vmem,
        compiler_params=room(8),
        name="total",
    )(parts)


def analysis_kernel(stack_ref, gathered_ref, out_ref, gram_ref, field_ref):
    n = LANES
    ens = 3 * n
    devices = gathered_ref.shape[0]
    members = ens // devices
    quads = members // 4
    row = lax.broadcasted_iota(jnp.int32, (n, n), 0)
    column = lax.broadcasted_iota(jnp.int32, (n, n), 1)

    def block(k):
        return stack_ref[k * n // 4 : (k + 1) * n // 4].reshape(n, n)

    for k, (i, j) in enumerate(((0, 1), (0, 2), (1, 2))):
        gram_ref[i * n : (i + 1) * n, j * n : (j + 1) * n] = block(k)
        gram_ref[j * n : (j + 1) * n, i * n : (i + 1) * n] = block(k).T
    both = block(3)
    upper = jnp.where(row < column, both, 0.0)
    gram_ref[0:n, 0:n] = upper + upper.T + jnp.where(row == column, both, 0.0)
    lower = jnp.where(row > column, both, 0.0)
    last = block(4)
    tail = last[n - 8 :]
    turned = pltpu.roll(tail, n // 2, 1)
    left = column[0:1] < n // 2
    vectors = [
        jnp.where(left, tail[2 * k : 2 * k + 1], turned[2 * k + 1 : 2 * k + 2]) for k in range(4)
    ]
    middle = jnp.where(row == column, vectors[0], 0.0)
    gram_ref[n : 2 * n, n : 2 * n] = lower + lower.T + middle
    upper = jnp.where(row < column, last, 0.0)
    gram_ref[2 * n :, 2 * n :] = upper + upper.T + jnp.where(row == column, last, 0.0)
    drive = jnp.concatenate(vectors[1:], axis=1)

    same = lax.broadcasted_iota(jnp.int32, (ens, ens), 0) == lax.broadcasted_iota(
        jnp.int32, (ens, ens), 1
    )
    identity = jnp.where(same, 1.0, 0.0)
    system = identity + gram_ref[...] * (1.0 / (ens - 1))
    norm_scale = jnp.sqrt(jnp.sum(system * system, keepdims=True))
    whole = system / norm_scale
    inverse = None
    for pair in range(NS_ITERS // 2):
        whole_halves = halves(whole)
        square = product(whole_halves, whole_halves)
        inner = 1.6875 * identity - 0.5625 * whole + 0.0625 * square
        quartic = product(halves(inner), halves(square)) + (2.25 * identity - 2.4375 * whole)
        quartic_halves = halves(quartic)
        inverse = quartic if pair == 0 else product(halves(inverse), quartic_halves)
        if 2 * pair + 2 < NS_ITERS:
            growth = product(quartic_halves, quartic_halves)
            whole = product(whole_halves, halves(growth))
    weights = inverse / jnp.sqrt(norm_scale)
    pulled = jnp.sum(weights * drive, axis=1, keepdims=True)
    mean_weight = jnp.sum(weights * pulled, axis=0, keepdims=True) * (1.0 / (ens - 1))
    combined = halves(weights + mean_weight)

    for f in range(3):
        for d in range(devices):
            field_ref[f, d * members : (d + 1) * members, :] = gathered_ref[
                d, f * GROUP : f * GROUP + members, :
            ]
    for f in range(3):
        field = field_ref[f]
        center = jnp.mean(field, axis=0, keepdims=True)
        field_ref[f] = center + product(combined, halves(field - center))
    for f in range(3):
        for d in range(devices):
            part = field_ref[f, d * members : (d + 1) * members, :]
            out_ref[d, f * quads : (f + 1) * quads] = part.reshape(quads, 4, n)


def analysis(stack, gathered):
    devices = gathered.shape[0]
    ens = 3 * LANES
    vmem = pl.BlockSpec(memory_space=pltpu.VMEM)
    return pl.pallas_call(
        analysis_kernel,
        out_shape=jax.ShapeDtypeStruct((devices, 3 * ens // devices // 4, 4, LANES), jnp.float32),
        in_specs=[vmem, vmem],
        out_specs=vmem,
        scratch_shapes=[
            pltpu.VMEM((ens, ens), jnp.float32),
            pltpu.VMEM((3, ens, LANES), jnp.float32),
        ],
        compiler_params=room(16),
        name="analysis",
    )(stack, gathered)


def local(ensemble, sea_depth, ocean_mask, observed_cells, observed_values, observed_error):
    local_members, fields, rows_here, columns = ensemble.shape
    devices = lax.axis_size(MEM)
    slabs = lax.axis_size("space")
    coriolis = 0.05 + 0.1 * jnp.arange(columns, dtype=jnp.float32)[None] / columns
    cells = observed_cells[0]
    places = jnp.stack(
        [
            cells // columns,
            cells % columns // LANES * LANES,
            (jnp.arange(LANES, dtype=jnp.int32) - cells) % LANES,
        ]
    )
    own = lax.axis_index(MEM).astype(jnp.int32).reshape(1)
    planes = planes_of(ensemble, sea_depth, ocean_mask)
    edge = HALO - rows_here
    before = lax.ppermute(planes, "space", ring("space", 1))
    after = lax.ppermute(planes, "space", ring("space", -1))
    far_before = lax.ppermute(planes[rows_here - edge :], "space", ring("space", 2))
    far_after = lax.ppermute(planes[:edge], "space", ring("space", -2))
    inner = inner_rows((before, planes, after), coriolis, local_members)
    pieces = (far_before, before, planes, after, far_after)
    sent = forecast(places, pieces, inner, coriolis, local_members, devices)
    gathered = lax.all_to_all(sent, MEM, 0, 0, tiled=True)
    parts = gram_piece(own, gathered, observed_values, observed_error, slabs)
    parts = lax.all_to_all(parts, "space", 0, 0, tiled=True)
    pieces = lax.all_to_all(total_piece(parts, devices), MEM, 0, 0, tiled=True)
    result = analysis(pieces.reshape(-1, 4, LANES), gathered)
    returned = lax.all_to_all(result, MEM, 0, 0, tiled=True)
    returned = returned.reshape(rows_here, columns // LANES, fields, local_members, LANES)
    return returned.transpose(3, 2, 0, 1, 4).reshape(ensemble.shape)


def solution(mesh):
    finer = Mesh(mesh.devices.reshape(8, 4, mesh.shape["space"]), ("mem_0", "mem_1", "space"))
    return jax.shard_map(
        local,
        mesh=finer,
        in_specs=(
            P(MEM, None, "space", None),
            P("space", None),
            P("space", None),
            P("space", None),
            P("space", None),
            P("space", None),
        ),
        out_specs=P(MEM, None, "space", None),
        check_vma=False,
    )
```
